8 devices in a mesh: dp: 2 (over z, y), pp: 4 (over x, core).
Axes of the slice: x: 2, y: 2, z: 1, core: 2. Of those that a mesh axis runs over, the one named last changes fastest.
Arguments:
- x_embed: bfloat16 [24, 512, 512], P('dp'), parts along dimension 0
- labels: int32 [24, 512], P('dp'), parts along dimension 0
- norm_gain: float32 [4, 2, 1, 512], P('pp')
- w_up: bfloat16 [4, 2, 1, 512, 2048], P('pp')
- w_down: bfloat16 [4, 2, 1, 2048, 512], P('pp')
- w_head: bfloat16 [50304, 512], P('pp')
Outputs:
- output 1: float32 [2], P('dp'), parts along dimension 0
- output 2: float32 [24, 512, 512], P(('dp', 'pp')), parts along dimension 0
- output 3: float32 [8, 2, 1, 512], P(('dp', 'pp')), parts along dimension 0
- output 4: bfloat16 [8, 2, 1, 512, 2048], P(('dp', 'pp')), parts along dimension 0
- output 5: bfloat16 [8, 2, 1, 2048, 512], P(('dp', 'pp')), parts along dimension 0
- output 6: bfloat16 [100608, 512], P(('dp', 'pp')), parts along dimension 0
There are 2 independent parts. The reference program is written for one: setup_inputs(seed, part) draws one part's arguments, and reference() takes and returns one part's arrays. A program takes and returns all parts, laid end to end along the dimension named above; an argument that names none is the same for every part.
All inputs are finite; a program needn't handle non-finite values.
Results may differ from the reference program's by a relative error of at most 0.02.
Values are sent between devices in bfloat16 or wider.
A program may use at most 1 GiB of HBM per device.

```python
import jax
import jax.numpy as jnp
from jax import lax

STAGES = 4
STAGE_LAYERS = 1
ROUNDS = 3
TOKENS = 512
D_MODEL = 512
D_FF = 2048
VOCAB_SIZE = 50304
NUM_MICRO = ROUNDS * STAGES
NUM_BLOCKS = 2 * STAGES * STAGE_LAYERS
NORM_EPS = 1e-6


def setup_inputs(seed: int = 0, part: int = 0) -> dict:
    base_key = jax.random.key(seed)
    part_key = jax.random.fold_in(base_key, part)
    key_x, key_lab = jax.random.split(part_key)
    key_gain, key_up, key_down, key_head = jax.random.split(jax.random.key(seed + 1), 4)
    x_embed = jax.random.normal(key_x, (NUM_MICRO, TOKENS, D_MODEL), jnp.float32).astype(jnp.bfloat16)
    labels = jax.random.randint(key_lab, (NUM_MICRO, TOKENS), 0, VOCAB_SIZE, jnp.int32)
    labels = labels.at[0, 0].set(0).at[0, 1].set(VOCAB_SIZE - 1)
    norm_gain = 1.0 + 0.3 * jax.random.normal(key_gain, (STAGES, 2, STAGE_LAYERS, D_MODEL), jnp.float32)
    w_up = (jax.random.normal(key_up, (STAGES, 2, STAGE_LAYERS, D_MODEL, D_FF), jnp.float32) * D_MODEL ** -0.5).astype(jnp.bfloat16)
    w_down = (jax.random.normal(key_down, (STAGES, 2, STAGE_LAYERS, D_FF, D_MODEL), jnp.float32) * D_FF ** -0.5).astype(jnp.bfloat16)
    head_ramp = (1.0 + 2.0 * jnp.arange(VOCAB_SIZE, dtype=jnp.float32) / VOCAB_SIZE)[:, None]
    w_head = (jax.random.normal(key_head, (VOCAB_SIZE, D_MODEL), jnp.float32) * head_ramp * D_MODEL ** -0.5).astype(jnp.bfloat16)
    return {'x_embed': x_embed, 'labels': labels, 'norm_gain': norm_gain, 'w_up': w_up, 'w_down': w_down, 'w_head': w_head}


def rms_scale(h_f32):
    return lax.rsqrt(jnp.mean(h_f32 * h_f32, axis=-1, keepdims=True) + NORM_EPS)


def block_apply(h_in, gain_vec, w_up, w_down):
    h_f32 = h_in.astype(jnp.float32)
    normed = (h_f32 * rms_scale(h_f32) * gain_vec).astype(jnp.bfloat16)
    hidden = jax.nn.gelu(jnp.dot(normed, w_up, preferred_element_type=jnp.float32)).astype(jnp.bfloat16)
    return (h_f32 + jnp.dot(hidden, w_down, preferred_element_type=jnp.float32)).astype(jnp.bfloat16)


def micro_loss(h_in, label_row, block_gains, block_ups, block_downs, w_head):
    def layer_body(h_cur, layer_params):
        return jax.checkpoint(block_apply)(h_cur, layer_params[0], layer_params[1], layer_params[2]), None
    h_last = lax.scan(layer_body, h_in, (block_gains, block_ups, block_downs))[0]
    h_f32 = h_last.astype(jnp.float32)
    h_norm = (h_f32 * rms_scale(h_f32)).astype(jnp.bfloat16)
    logits = jnp.dot(h_norm, w_head.T, preferred_element_type=jnp.float32)
    log_norm = jax.nn.logsumexp(logits, axis=-1)
    target = jnp.take_along_axis(logits, label_row[:, None], axis=-1)[:, 0]
    return jnp.sum(log_norm - target) / (NUM_MICRO * TOKENS)


def model_order(stacked):
    return jnp.swapaxes(stacked, 0, 1).reshape((NUM_BLOCKS,) + stacked.shape[3:])


def stage_order(flat_arr):
    return jnp.swapaxes(flat_arr.reshape((2, STAGES, STAGE_LAYERS) + flat_arr.shape[1:]), 0, 1)


def reference(x_embed, labels, norm_gain, w_up, w_down, w_head):
    block_gains = model_order(norm_gain)
    block_ups = model_order(w_up)
    block_downs = model_order(w_down)
    grad_fn = jax.value_and_grad(micro_loss, argnums=(0, 2, 3, 4, 5))

    def micro_step(acc_state, micro_in):
        micro_val, grad_set = grad_fn(micro_in[0], micro_in[1], block_gains, block_ups, block_downs, w_head)
        new_state = (acc_state[0] + micro_val, acc_state[1] + grad_set[1], acc_state[2] + grad_set[2].astype(jnp.float32), acc_state[3] + grad_set[3].astype(jnp.float32), acc_state[4] + grad_set[4].astype(jnp.float32))
        return new_state, grad_set[0].astype(jnp.float32)

    init_state = (jnp.zeros((), jnp.float32), jnp.zeros(block_gains.shape, jnp.float32), jnp.zeros(block_ups.shape, jnp.float32), jnp.zeros(block_downs.shape, jnp.float32), jnp.zeros(w_head.shape, jnp.float32))
    final_state, d_embed = lax.scan(micro_step, init_state, (x_embed, labels))
    return (final_state[0].reshape(1), d_embed, stage_order(final_state[1]), stage_order(final_state[2]).astype(jnp.bfloat16), stage_order(final_state[3]).astype(jnp.bfloat16), final_state[4].astype(jnp.bfloat16))
```

```python
import functools

import jax
import jax.numpy as jnp
from jax import lax
from jax.experimental import pallas as pl
from jax.experimental.pallas import tpu as pltpu
from jax.sharding import PartitionSpec as P

NORM_EPS = 1e-6
VMEM_MAX = 67_000_000
GELU_A = 0.7978845608028654
GELU_B = GELU_A * 0.044715
SUB = 1024

ANY = pl.BlockSpec(memory_space=pl.ANY)
VMEM = pl.BlockSpec(memory_space=pltpu.VMEM)


def nn(lhs, rhs):
    return lax.dot_general(lhs, rhs, (((1,), (0,)), ((), ())), preferred_element_type=jnp.float32)


def nt(lhs, rhs):
    return lax.dot_general(lhs, rhs, (((1,), (1,)), ((), ())), preferred_element_type=jnp.float32)


def col_scale(h_f32):
    return lax.rsqrt(jnp.mean(h_f32 * h_f32, axis=0, keepdims=True) + NORM_EPS)


def gelu_pair(x):
    x2 = x * x
    th = jnp.tanh(x * (GELU_A + GELU_B * x2))
    hx = 0.5 * x
    slope = 0.5 + 0.5 * th + hx * (1.0 - th * th) * (GELU_A + (3.0 * GELU_B) * x2)
    return hx + hx * th, slope


def group_barrier(me, n_stage):
    sem = pltpu.get_barrier_semaphore()
    for step in range(1, n_stage):
        pl.semaphore_signal(sem, inc=1, device_id={"pp": lax.rem(me + step, n_stage)}, device_id_type=pl.DeviceIdType.MESH)
    pl.semaphore_wait(sem, n_stage - 1)


def remote(src, dst, send_sem, recv_sem, dev):
    return pltpu.make_async_remote_copy(src_ref=src, dst_ref=dst, send_sem=send_sem, recv_sem=recv_sem, device_id={"pp": dev}, device_id_type=pl.DeviceIdType.MESH)


def fwd_kernel(n_stage, num_micro, x_ref, g_ref, w1t_ref, w2t_ref, saved_ref, slope_ref, hid_ref, hfin_ref,
               hbuf, obuf, fbuf, slope_st, hid_st, in_sem, out_sem, save_sem, slope_sem, hid_sem, fin_sem, fin_a, fin_b, fin_c):
    me = lax.axis_index("pp")
    right = lax.rem(me + 1, n_stage)
    first, last = me == 0, me == n_stage - 1
    n_unit = 2 * num_micro
    d_ff = w1t_ref.shape[1]
    group_barrier(me, n_stage)

    @pl.when(first)
    def _():
        @pl.loop(0, num_micro)
        def _(m):
            pltpu.make_async_copy(x_ref.at[m], hbuf.at[m], in_sem.at[m]).start()

    @pl.loop(0, n_unit)
    def _(u):
        half = u // num_micro
        m = lax.rem(u, num_micro)
        from_x = first & (half == 0)
        is_final = last & (half == 1)
        par = lax.rem(u, 2)

        @pl.when(from_x)
        def _():
            pltpu.make_async_copy(x_ref.at[m], hbuf.at[u], in_sem.at[u]).wait()

        @pl.when(jnp.logical_not(from_x))
        def _():
            remote(obuf.at[0], hbuf.at[u], out_sem.at[0], in_sem.at[u], right).wait_recv()

        pltpu.make_async_copy(hbuf.at[u], saved_ref.at[u], save_sem.at[u]).start()

        @pl.when(u >= 2)
        def _():
            pltpu.make_async_copy(slope_st.at[par], slope_ref.at[u - 2], slope_sem.at[par]).wait()
            pltpu.make_async_copy(hid_st.at[par], hid_ref.at[u - 2], hid_sem.at[par]).wait()

        h = hbuf[u].astype(jnp.float32)
        y = (h * col_scale(h) * g_ref[half]).astype(jnp.bfloat16)
        step = 512
        for k in range(d_ff // step):
            rows = pl.ds(k * step, step)
            hid, slope = gelu_pair(nn(w1t_ref[half, rows, :], y))
            hid_st[par, rows, :] = hid.astype(jnp.bfloat16)
            slope_st[par, rows, :] = slope
        out = (h + nn(w2t_ref[half], hid_st[par])).astype(jnp.bfloat16)
        pltpu.make_async_copy(slope_st.at[par], slope_ref.at[u], slope_sem.at[par]).start()
        pltpu.make_async_copy(hid_st.at[par], hid_ref.at[u], hid_sem.at[par]).start()

        @pl.when(is_final)
        def _():
            fbuf[m] = out
            pltpu.make_async_copy(fbuf.at[m], hfin_ref.at[m], fin_c.at[m]).start()
            remote(fbuf.at[m], hfin_ref.at[m], fin_a.at[m], fin_sem.at[m], n_stage - 2).start()
            remote(fbuf.at[m], hfin_ref.at[m], fin_b.at[m], fin_sem.at[m], 1).start()

        @pl.when(jnp.logical_not(is_final))
        def _():
            slot = lax.rem(u, 4)

            @pl.when(u >= 4)
            def _():
                remote(obuf.at[slot], hbuf.at[u], out_sem.at[slot], in_sem.at[u], right).wait_send()

            obuf[slot] = out
            dst = u + jnp.where(last, num_micro, 0)
            remote(obuf.at[slot], hbuf.at[dst], out_sem.at[slot], in_sem.at[dst], right).start()

    for slot in range(4):
        remote(obuf.at[slot], hbuf.at[0], out_sem.at[slot], in_sem.at[0], right).wait_send()
    for par in range(2):
        pltpu.make_async_copy(slope_st.at[par], slope_ref.at[par], slope_sem.at[par]).wait()
        pltpu.make_async_copy(hid_st.at[par], hid_ref.at[par], hid_sem.at[par]).wait()

    @pl.loop(0, n_unit)
    def _(u):
        pltpu.make_async_copy(hbuf.at[u], saved_ref.at[u], save_sem.at[u]).wait()

    @pl.when(last)
    def _():
        @pl.loop(0, num_micro)
        def _(m):
            pltpu.make_async_copy(fbuf.at[m], hfin_ref.at[m], fin_c.at[m]).wait()
            remote(fbuf.at[m], hfin_ref.at[m], fin_a.at[m], fin_sem.at[m], n_stage - 2).wait_send()
            remote(fbuf.at[m], hfin_ref.at[m], fin_b.at[m], fin_sem.at[m], 1).wait_send()

    @pl.when(jnp.logical_not(last))
    def _():
        @pl.loop(0, num_micro)
        def _(m):
            remote(fbuf.at[m], hfin_ref.at[m], fin_a.at[m], fin_sem.at[m], right).wait_recv()

            @pl.when(me == 1)
            def _():
                remote(hfin_ref.at[m], hfin_ref.at[m], fin_a.at[m], fin_sem.at[m], 0).start()

    @pl.when(me == 1)
    def _():
        @pl.loop(0, num_micro)
        def _(m):
            remote(hfin_ref.at[m], hfin_ref.at[m], fin_a.at[m], fin_sem.at[m], 0).wait_send()


def run_forward(x_t, gains, w1t, w2t, n_stage):
    num_micro, d_model, tokens = x_t.shape
    d_ff = w1t.shape[1]
    bf, f32 = jnp.bfloat16, jnp.float32
    n_unit = 2 * num_micro
    dma = pltpu.SemaphoreType.DMA
    return pl.pallas_call(
        functools.partial(fwd_kernel, n_stage, num_micro),
        name="stack_fwd",
        out_shape=(jax.ShapeDtypeStruct((n_unit, d_model, tokens), bf), jax.ShapeDtypeStruct((n_unit, d_ff, tokens), f32),
                   jax.ShapeDtypeStruct((n_unit, d_ff, tokens), bf), jax.ShapeDtypeStruct((num_micro, d_model, tokens), bf)),
        in_specs=[ANY, VMEM, VMEM, VMEM],
        out_specs=(ANY, ANY, ANY, ANY),
        scratch_shapes=[
            pltpu.VMEM((n_unit, d_model, tokens), bf), pltpu.VMEM((4, d_model, tokens), bf), pltpu.VMEM((num_micro, d_model, tokens), bf),
            pltpu.VMEM((2, d_ff, tokens), f32), pltpu.VMEM((2, d_ff, tokens), bf),
            dma((n_unit,)), dma((4,)), dma((n_unit,)), dma((2,)), dma((2,)), dma((num_micro,)), dma((num_micro,)), dma((num_micro,)), dma((num_micro,)),
        ],
        compiler_params=pltpu.CompilerParams(collective_id=0, has_side_effects=True, vmem_limit_bytes=VMEM_MAX),
        cost_estimate=pl.CostEstimate(flops=4 * n_unit * tokens * d_model * d_ff, bytes_accessed=7 * n_unit * d_ff * tokens, transcendentals=0),
    )(x_t, gains, w1t, w2t)


def sub_tiles(tile):
    n_sub = tile // SUB
    return [(k * SUB, SUB if k + 1 < n_sub else tile - k * SUB) for k in range(n_sub)]


def logits_kernel(h_ref, lab_ref, w_ref, e_ref, mrun_ref, stat_ref, n_ref, run):
    j = pl.program_id(1)
    tile = e_ref.shape[1]
    subs = sub_tiles(tile)

    @pl.when(j == 0)
    def _():
        run[0:1, :] = jnp.full((1, run.shape[1]), -jnp.inf, jnp.float32)
        run[1:3, :] = jnp.zeros((2, run.shape[1]), jnp.float32)
        h = h_ref[0].astype(jnp.float32)
        n_ref[0] = (h * col_scale(h)).astype(jnp.bfloat16)

    n = n_ref[0]
    lab = lab_ref[0] - j * tile
    m_run, s_run, z_lab = run[0:1, :], run[1:2, :], run[2:3, :]
    for k, (off, size) in enumerate(subs):
        z = nn(w_ref[pl.ds(pl.multiple_of(j * tile + off, 16), size), :], n)
        m_new = jnp.maximum(m_run, jnp.max(z, axis=0, keepdims=True))
        e = jnp.exp(z - m_new)
        e_ref[0, off:off + size, :] = e.astype(jnp.bfloat16)
        s_run = s_run * jnp.exp(m_run - m_new) + jnp.sum(e, axis=0, keepdims=True)
        hit = lax.broadcasted_iota(jnp.int32, z.shape, 0) == lab - off
        z_lab = z_lab + jnp.sum(jnp.where(hit, z, 0.0), axis=0, keepdims=True)
        m_run = m_new
        mrun_ref[0, pl.ds(j * len(subs) + k, 1), :] = m_run
    run[0:1, :] = m_run
    run[1:2, :] = s_run
    run[2:3, :] = z_lab
    stat_ref[0] = run[...]


def d_logits(e_tile, fac_row, lab, off, inv):
    hit = lax.broadcasted_iota(jnp.int32, e_tile.shape, 0) == lab - off
    return (e_tile.astype(jnp.float32) * fac_row - jnp.where(hit, inv, 0.0)).astype(jnp.bfloat16)


def dnorm_kernel(inv, e_ref, fac_ref, lab_ref, wt_ref, dn_ref):
    j = pl.program_id(1)
    tile = e_ref.shape[1]
    subs = sub_tiles(tile)
    lab = lab_ref[0] - j * tile
    total = None
    for k, (off, size) in enumerate(subs):
        d = d_logits(e_ref[0, off:off + size, :], fac_ref[0, pl.ds(j * len(subs) + k, 1), :], lab, off, inv)
        part = nn(wt_ref[j, :, off:off + size], d)
        total = part if total is None else total + part

    @pl.when(j == 0)
    def _():
        dn_ref[0] = total

    @pl.when(j > 0)
    def _():
        dn_ref[0] += total


def dhead_kernel(inv, e_ref, fac_ref, lab_ref, n_ref, out_ref, acc):
    j, i = pl.program_id(0), pl.program_id(1)
    tile = e_ref.shape[1]
    subs = sub_tiles(tile)
    per = e_ref.shape[0]

    @pl.when(i == 0)
    def _():
        acc[...] = jnp.zeros_like(acc)

    for k, (off, size) in enumerate(subs):
        total = None
        for b in range(per):
            d = d_logits(e_ref[b, off:off + size, :], fac_ref[b, pl.ds(j * len(subs) + k, 1), :], lab_ref[b] - j * tile, off, inv)
            part = nt(d, n_ref[b])
            total = part if total is None else total + part
        acc[off:off + size, :] += total

    @pl.when(i == pl.num_programs(1) - 1)
    def _():
        out_ref[...] = acc[...].astype(jnp.bfloat16)


def run_head(h_fin, labels, w_head, stage_id, n_stage):
    num_micro, d_model, tokens = h_fin.shape
    vocab = w_head.shape[0]
    n_tile = 3
    tile = vocab // n_tile
    n_row = 16
    bf, f32 = jnp.bfloat16, jnp.float32
    inv = 1.0 / (num_micro * tokens)
    lab = (labels - stage_id * vocab).reshape(num_micro, 1, tokens)
    params = pltpu.CompilerParams(vmem_limit_bytes=VMEM_MAX)
    flops = 2 * num_micro * tokens * d_model * vocab
    e_bytes = 2 * num_micro * tokens * vocab

    def cost(extra):
        return pl.CostEstimate(flops=flops, bytes_accessed=e_bytes + extra, transcendentals=0)

    micro3 = lambda shape: pl.BlockSpec(shape, lambda i, j: (i, 0, 0))
    e, m_run, stat, n_t = pl.pallas_call(
        logits_kernel, name="head_logits",
        grid=(num_micro, n_tile),
        out_shape=(jax.ShapeDtypeStruct((num_micro, vocab, tokens), bf), jax.ShapeDtypeStruct((num_micro, n_row, tokens), f32),
                   jax.ShapeDtypeStruct((num_micro, 8, tokens), f32), jax.ShapeDtypeStruct((num_micro, d_model, tokens), bf)),
        in_specs=[micro3((1, d_model, tokens)), micro3((1, 1, tokens)), VMEM],
        out_specs=(pl.BlockSpec((1, tile, tokens), lambda i, j: (i, j, 0)), micro3((1, n_row, tokens)), micro3((1, 8, tokens)), micro3((1, d_model, tokens))),
        scratch_shapes=[pltpu.VMEM((8, tokens), f32)],
        compiler_params=params, cost_estimate=cost(0),
    )(h_fin, lab, w_head)

    stats = lax.all_gather(stat[:, :3, :], 'pp')
    m_all, s_all = stats[:, :, 0], stats[:, :, 1]
    m_top = jnp.max(m_all, axis=0)
    s_top = jnp.sum(s_all * jnp.exp(m_all - m_top), axis=0)
    loss = jnp.sum(m_top + jnp.log(s_top) - jnp.sum(stats[:, :, 2], axis=0)) * inv
    fac = jnp.exp(m_run - m_top[:, None, :]) * (inv / s_top)[:, None, :]

    wt = jnp.swapaxes(w_head.reshape(n_tile, tile, d_model), 1, 2)
    dn = pl.pallas_call(
        functools.partial(dnorm_kernel, inv), name="head_dnorm",
        grid=(num_micro, n_tile),
        out_shape=jax.ShapeDtypeStruct((num_micro, d_model, tokens), f32),
        in_specs=[pl.BlockSpec((1, tile, tokens), lambda i, j: (i, j, 0)), micro3((1, n_row, tokens)), micro3((1, 1, tokens)), VMEM],
        out_specs=micro3((1, d_model, tokens)),
        compiler_params=params, cost_estimate=cost(0),
    )(e, fac, lab, wt)

    per = 2
    head_grad = pl.pallas_call(
        functools.partial(dhead_kernel, inv), name="head_dweight",
        grid=(n_tile, num_micro // per),
        out_shape=jax.ShapeDtypeStruct((vocab, d_model), bf),
        in_specs=[pl.BlockSpec((per, tile, tokens), lambda j, i: (i, j, 0)), pl.BlockSpec((per, n_row, tokens), lambda j, i: (i, 0, 0)),
                  pl.BlockSpec((per, 1, tokens), lambda j, i: (i, 0, 0)), pl.BlockSpec((per, d_model, tokens), lambda j, i: (i, 0, 0))],
        out_specs=pl.BlockSpec((tile, d_model), lambda j, i: (j, 0)),
        scratch_shapes=[pltpu.VMEM((tile, d_model), f32)],
        compiler_params=params, cost_estimate=cost(0),
    )(e, fac, lab, n_t)

    dn_own = lax.psum_scatter(dn, 'pp', scatter_dimension=0, tiled=True)
    per_stage = num_micro // n_stage
    h_own = lax.dynamic_slice_in_dim(h_fin, stage_id * per_stage, per_stage, 0).astype(f32)
    r_own = lax.rsqrt(jnp.mean(h_own * h_own, axis=1, keepdims=True) + NORM_EPS)
    n_own = h_own * r_own
    d_fin = r_own * (dn_own - n_own * jnp.mean(dn_own * n_own, axis=1, keepdims=True))
    return loss, head_grad, d_fin.astype(bf)


def bwd_kernel(n_stage, num_micro, dfin_ref, saved_ref, slope_ref, hid_ref, g_ref, w1_ref, w2_ref, dw1_ref, dw2_ref, dg_ref, dx_ref,
               dbuf, obuf, xbuf, h_in, slope_in, hid_in, dpre, acc1, acc2, accg, st1, st2,
               in_sem, push_sem, out_sem, x_sem, xr_sem, h_sem, slope_sem, hid_sem, w_sem):
    me = lax.axis_index("pp")
    left = lax.rem(me + n_stage - 1, n_stage)
    first, last = me == 0, me == n_stage - 1
    n_unit = 2 * num_micro
    per = num_micro // n_stage
    d_ff = w1_ref.shape[2]
    step = 512
    group_barrier(me, n_stage)

    def fetch(w):
        u, par = n_unit - 1 - w, lax.rem(w, 2)
        return (pltpu.make_async_copy(saved_ref.at[u], h_in.at[par], h_sem.at[par]),
                pltpu.make_async_copy(slope_ref.at[u], slope_in.at[par], slope_sem.at[par]),
                pltpu.make_async_copy(hid_ref.at[u], hid_in.at[par], hid_sem.at[par]))

    for copy in fetch(0):
        copy.start()

    @pl.when(last)
    def _():
        for i in range(per):
            slot = num_micro - 1 - (per * (n_stage - 1) + i)
            pltpu.make_async_copy(dfin_ref.at[i], dbuf.at[slot], in_sem.at[slot]).start()

    @pl.when(jnp.logical_not(last))
    def _():
        for i in reversed(range(per)):
            slot = num_micro - 1 - (per * me + i)
            remote(dfin_ref.at[i], dbuf.at[slot], push_sem.at[i], in_sem.at[slot], n_stage - 1).start()

    @pl.loop(0, n_unit)
    def _(w):
        half = 1 - w // num_micro
        par = lax.rem(w, 2)
        is_local = last & (w < per)
        is_final = first & (half == 0)

        @pl.when(w + 1 < n_unit)
        def _():
            for copy in fetch(w + 1):
                copy.start()

        @pl.when(lax.rem(w, num_micro) == 0)
        def _():
            acc1[...] = jnp.zeros_like(acc1)
            acc2[...] = jnp.zeros_like(acc2)
            accg[...] = jnp.zeros_like(accg)

        @pl.when(is_local)
        def _():
            pltpu.make_async_copy(dfin_ref.at[0], dbuf.at[w], in_sem.at[w]).wait()

        @pl.when(jnp.logical_not(is_local))
        def _():
            remote(obuf.at[0], dbuf.at[w], out_sem.at[0], in_sem.at[w], left).wait_recv()

        for copy in fetch(w):
            copy.wait()

        d_in = dbuf[w]
        for k in range(d_ff // step):
            rows = pl.ds(k * step, step)
            dpre[rows, :] = (nn(w2_ref[half, rows, :], d_in) * slope_in[par, rows, :]).astype(jnp.bfloat16)
        d_y = nn(w1_ref[half], dpre[...])
        h = h_in[par].astype(jnp.float32)
        r = col_scale(h)
        hr = h * r
        gain = g_ref[half]
        accg[...] += d_y * hr
        d_t = d_y * gain
        d_out = d_in.astype(jnp.float32) + r * (d_t - hr * jnp.mean(d_t * hr, axis=0, keepdims=True))

        @pl.when(is_final)
        def _():
            q = w - num_micro
            slot = lax.rem(q, 4)
            m = num_micro - 1 - q
            owner, i = m // per, lax.rem(m, per)

            @pl.when(q >= 4)
            def _():
                remote(xbuf.at[slot], dx_ref.at[0], x_sem.at[slot], xr_sem.at[0], left).wait_send()

            xbuf[slot] = d_out

            @pl.when(owner == 0)
            def _():
                pltpu.make_async_copy(xbuf.at[slot], dx_ref.at[i], x_sem.at[slot]).start()

            @pl.when(owner > 0)
            def _():
                remote(xbuf.at[slot], dx_ref.at[i], x_sem.at[slot], xr_sem.at[i], jnp.maximum(owner, 1)).start()

        @pl.when(jnp.logical_not(is_final))
        def _():
            slot = lax.rem(w, 4)

            @pl.when(w >= 4)
            def _():
                remote(obuf.at[slot], dbuf.at[w], out_sem.at[slot], in_sem.at[w], left).wait_send()

            obuf[slot] = d_out.astype(jnp.bfloat16)
            dst = w + jnp.where(first, num_micro, 0)
            remote(obuf.at[slot], dbuf.at[dst], out_sem.at[slot], in_sem.at[dst], left).start()

        y = (hr * gain).astype(jnp.bfloat16)
        for k in range(d_ff // step):
            rows = pl.ds(k * step, step)
            acc2[rows, :] += nt(hid_in[par, rows, :], d_in)
            acc1[:, rows] += nt(y, dpre[rows, :])

        @pl.when(lax.rem(w, num_micro) == num_micro - 1)
        def _():
            @pl.when(half == 0)
            def _():
                pltpu.make_async_copy(st1, dw1_ref.at[1], w_sem.at[0]).wait()
                pltpu.make_async_copy(st2, dw2_ref.at[1], w_sem.at[1]).wait()

            st1[...] = acc1[...].astype(jnp.bfloat16)
            st2[...] = acc2[...].astype(jnp.bfloat16)
            dg_ref[half] = jnp.sum(accg[...], axis=1, keepdims=True)
            pltpu.make_async_copy(st1, dw1_ref.at[half], w_sem.at[0]).start()
            pltpu.make_async_copy(st2, dw2_ref.at[half], w_sem.at[1]).start()

    pltpu.make_async_copy(st1, dw1_ref.at[0], w_sem.at[0]).wait()
    pltpu.make_async_copy(st2, dw2_ref.at[0], w_sem.at[1]).wait()
    for slot in range(4):
        remote(obuf.at[slot], dbuf.at[0], out_sem.at[slot], in_sem.at[0], left).wait_send()

    @pl.when(jnp.logical_not(last))
    def _():
        for i in range(per):
            remote(dfin_ref.at[i], dbuf.at[0], push_sem.at[i], in_sem.at[0], n_stage - 1).wait_send()

    @pl.when(first)
    def _():
        remote(xbuf.at[0], dx_ref.at[0], x_sem.at[0], xr_sem.at[0], left).wait_send()
        for slot in range(1, 4):
            pltpu.make_async_copy(xbuf.at[slot], dx_ref.at[0], x_sem.at[slot]).wait()

    @pl.when(jnp.logical_not(first))
    def _():
        for i in range(per):
            remote(xbuf.at[0], dx_ref.at[i], x_sem.at[0], xr_sem.at[i], left).wait_recv()


def run_backward(d_fin, saved, slope, hid, gains, w1, w2, n_stage):
    n_unit, d_model, tokens = saved.shape
    num_micro = n_unit // 2
    d_ff = w1.shape[2]
    per = num_micro // n_stage
    bf, f32 = jnp.bfloat16, jnp.float32
    dma = pltpu.SemaphoreType.DMA
    return pl.pallas_call(
        functools.partial(bwd_kernel, n_stage, num_micro),
        name="stack_bwd",
        out_shape=(jax.ShapeDtypeStruct(w1.shape, bf), jax.ShapeDtypeStruct(w2.shape, bf), jax.ShapeDtypeStruct((2, d_model, 1), f32),
                   jax.ShapeDtypeStruct((per, d_model, tokens), f32)),
        in_specs=[ANY, ANY, ANY, ANY, VMEM, VMEM, VMEM],
        out_specs=(ANY, ANY, VMEM, ANY),
        scratch_shapes=[
            pltpu.VMEM((n_unit, d_model, tokens), bf), pltpu.VMEM((4, d_model, tokens), bf), pltpu.VMEM((4, d_model, tokens), f32),
            pltpu.VMEM((2, d_model, tokens), bf), pltpu.VMEM((2, d_ff, tokens), f32), pltpu.VMEM((2, d_ff, tokens), bf),
            pltpu.VMEM((d_ff, tokens), bf), pltpu.VMEM((d_model, d_ff), f32), pltpu.VMEM((d_ff, d_model), f32), pltpu.VMEM((d_model, tokens), f32),
            pltpu.VMEM((d_model, d_ff), bf), pltpu.VMEM((d_ff, d_model), bf),
            dma((n_unit,)), dma((per,)), dma((4,)), dma((4,)), dma((per,)), dma((2,)), dma((2,)), dma((2,)), dma((2,)),
        ],
        compiler_params=pltpu.CompilerParams(collective_id=1, has_side_effects=True, vmem_limit_bytes=VMEM_MAX),
        cost_estimate=pl.CostEstimate(flops=8 * n_unit * tokens * d_model * d_ff, bytes_accessed=7 * n_unit * d_ff * tokens, transcendentals=0),
    )(d_fin, saved, slope, hid, gains, w1, w2)


def solution(mesh):
    n_stage = mesh.shape['pp']

    def local_step(x_embed, labels, norm_gain, w_up, w_down, w_head):
        stage_id = lax.axis_index('pp')
        gains = jnp.swapaxes(norm_gain[0], 1, 2)
        w1, w2 = w_up[0, :, 0], w_down[0, :, 0]
        saved, slope, hid, h_fin = run_forward(jnp.swapaxes(x_embed, 1, 2), gains, jnp.swapaxes(w1, 1, 2), jnp.swapaxes(w2, 1, 2), n_stage)
        loss, head_grad, d_fin = run_head(h_fin, labels, w_head, stage_id, n_stage)
        dw1, dw2, dg, dx = run_backward(d_fin, saved, slope, hid, gains, w1, w2, n_stage)
        return (loss.reshape(1), jnp.swapaxes(dx, 1, 2), jnp.swapaxes(dg, 1, 2)[None], dw1[None, :, None], dw2[None, :, None], head_grad)

    part_spec = P('dp')
    stage_spec = P('pp')
    out_spec = P(('dp', 'pp'))
    return jax.shard_map(local_step, mesh=mesh, in_specs=(part_spec, part_spec, stage_spec, stage_spec, stage_spec, stage_spec), out_specs=(part_spec, out_spec, out_spec, out_spec, out_spec, out_spec), check_vma=False)
```

```python
import functools

import jax
import jax.numpy as jnp
from jax import lax
from jax.experimental import pallas as pl
from jax.experimental.pallas import tpu as pltpu
from jax.sharding import PartitionSpec as P

NORM_EPS = 1e-6
VMEM_MAX = 67_000_000
GELU_A = 0.7978845608028654
GELU_B = GELU_A * 0.044715
SUB = 1024

ANY = pl.BlockSpec(memory_space=pl.ANY)
VMEM = pl.BlockSpec(memory_space=pltpu.VMEM)


def nn(lhs, rhs):
    return lax.dot_general(lhs, rhs, (((1,), (0,)), ((), ())), preferred_element_type=jnp.float32)


def nt(lhs, rhs):
    return lax.dot_general(lhs, rhs, (((1,), (1,)), ((), ())), preferred_element_type=jnp.float32)


def col_scale(h_f32):
    return lax.rsqrt(jnp.mean(h_f32 * h_f32, axis=0, keepdims=True) + NORM_EPS)


def gelu_pair(x):
    x2 = x * x
    th = jnp.tanh(x * (GELU_A + GELU_B * x2))
    hx = 0.5 * x
    slope = 0.5 + 0.5 * th + hx * (1.0 - th * th) * (GELU_A + (3.0 * GELU_B) * x2)
    return hx + hx * th, slope


def group_barrier(me, n_stage):
    sem = pltpu.get_barrier_semaphore()
    for step in range(1, n_stage):
        pl.semaphore_signal(sem, inc=1, device_id={"pp": lax.rem(me + step, n_stage)}, device_id_type=pl.DeviceIdType.MESH)
    pl.semaphore_wait(sem, n_stage - 1)


def remote(src, dst, send_sem, recv_sem, dev):
    return pltpu.make_async_remote_copy(src_ref=src, dst_ref=dst, send_sem=send_sem, recv_sem=recv_sem, device_id={"pp": dev}, device_id_type=pl.DeviceIdType.MESH)


def fwd_kernel(n_stage, num_micro, x_ref, g_ref, w1_ref, w2_ref, wh_ref, saved_ref, slope_ref, hid_ref, hfin_ref, n_ref, wht_ref,
               w1t, w2t, hbuf, obuf, fbuf, slope_st, hid_st, wh_in, wh_out, wh_last, wht_last, in_sem, out_sem, save_sem, slope_sem, hid_sem, fin_sem, fin_a, fin_b, fin_c, whi_sem, who_sem):
    me = lax.axis_index("pp")
    right = lax.rem(me + 1, n_stage)
    first, last = me == 0, me == n_stage - 1
    n_unit = 2 * num_micro
    d_ff = w1_ref.shape[2]
    n_tile, tile = wht_ref.shape[0], wht_ref.shape[2]
    subs = sub_tiles(tile)
    group_barrier(me, n_stage)

    def emit_norm(m):
        hf = fbuf[m].astype(jnp.float32)
        hbuf[m] = (hf * col_scale(hf)).astype(jnp.bfloat16)
        pltpu.make_async_copy(hbuf.at[m], n_ref.at[m], save_sem.at[m]).start()

    def head_copies(t, k):
        off, size = subs[k]
        last_sub = k + 1 == len(subs)
        src, dst = (wh_last, wht_last) if last_sub else (wh_in, wh_out)
        rows = pl.ds(pl.multiple_of(t * tile + off, 16), size)
        return (src, dst, pltpu.make_async_copy(wh_ref.at[rows, :], src, whi_sem.at[int(last_sub)]),
                pltpu.make_async_copy(dst, wht_ref.at[t, :, off:off + size], who_sem.at[int(last_sub)]))

    @pl.when(first)
    def _():
        @pl.loop(0, num_micro)
        def _(m):
            pltpu.make_async_copy(x_ref.at[m], hbuf.at[m], in_sem.at[m]).start()

    @pl.loop(0, n_unit)
    def _(u):
        half = u // num_micro

        @pl.when(lax.rem(u, num_micro) == 0)
        def _():
            w1t[...] = w1_ref[half].T
            w2t[...] = w2_ref[half].T

        m = lax.rem(u, num_micro)
        from_x = first & (half == 0)
        is_final = last & (half == 1)
        par = lax.rem(u, 2)

        @pl.when(from_x)
        def _():
            pltpu.make_async_copy(x_ref.at[m], hbuf.at[u], in_sem.at[u]).wait()
            hbuf[u] = hbuf[u].T

        @pl.when(jnp.logical_not(from_x))
        def _():
            remote(obuf.at[0], hbuf.at[u], out_sem.at[0], in_sem.at[u], right).wait_recv()

        pltpu.make_async_copy(hbuf.at[u], saved_ref.at[u], save_sem.at[u]).start()

        @pl.when(u >= 2)
        def _():
            pltpu.make_async_copy(slope_st.at[par], slope_ref.at[u - 2], slope_sem.at[par]).wait()
            pltpu.make_async_copy(hid_st.at[par], hid_ref.at[u - 2], hid_sem.at[par]).wait()

        h = hbuf[u].astype(jnp.float32)
        y = (h * col_scale(h) * g_ref[half]).astype(jnp.bfloat16)
        step = 512
        pre = nn(w1t[0:step, :], y)
        for k in range(d_ff // step):
            rows = pl.ds(k * step, step)
            cur = pre
            if k + 1 < d_ff // step:
                pre = nn(w1t[(k + 1) * step:(k + 2) * step, :], y)
            hid, slope = gelu_pair(cur)
            hid_st[par, rows, :] = hid.astype(jnp.bfloat16)
            slope_st[par, rows, :] = slope
        out = (h + nn(w2t[...], hid_st[par])).astype(jnp.bfloat16)
        pltpu.make_async_copy(slope_st.at[par], slope_ref.at[u], slope_sem.at[par]).start()
        pltpu.make_async_copy(hid_st.at[par], hid_ref.at[u], hid_sem.at[par]).start()

        @pl.when(is_final)
        def _():
            fbuf[m] = out
            pltpu.make_async_copy(fbuf.at[m], hfin_ref.at[m], fin_c.at[m]).start()
            remote(fbuf.at[m], fbuf.at[m], fin_a.at[m], fin_sem.at[m], n_stage - 2).start()
            remote(fbuf.at[m], fbuf.at[m], fin_b.at[m], fin_sem.at[m], 1).start()
            pltpu.make_async_copy(hbuf.at[m], saved_ref.at[m], save_sem.at[m]).wait()
            emit_norm(m)

        @pl.when(jnp.logical_not(is_final))
        def _():
            slot = lax.rem(u, 4)

            @pl.when(u >= 4)
            def _():
                remote(obuf.at[slot], hbuf.at[u], out_sem.at[slot], in_sem.at[u], right).wait_send()

            obuf[slot] = out
            dst = u + jnp.where(last, num_micro, 0)
            remote(obuf.at[slot], hbuf.at[dst], out_sem.at[slot], in_sem.at[dst], right).start()

        for k in range(len(subs)):
            @pl.when((lax.rem(u, 2 * len(subs)) == 2 * k) & (u // (2 * len(subs)) < n_tile))
            def _(k=k):
                head_copies(u // (2 * len(subs)), k)[2].start()

            @pl.when((lax.rem(u, 2 * len(subs)) == 2 * k + 1) & (u // (2 * len(subs)) < n_tile))
            def _(k=k):
                t = u // (2 * len(subs))
                src, dst, copy_in, copy_out = head_copies(t, k)
                copy_in.wait()
                dst[...] = src[...].T
                copy_out.start()
                copy_out.wait()

    for slot in range(4):
        remote(obuf.at[slot], hbuf.at[0], out_sem.at[slot], in_sem.at[0], right).wait_send()
    for par in range(2):
        pltpu.make_async_copy(slope_st.at[par], slope_ref.at[par], slope_sem.at[par]).wait()
        pltpu.make_async_copy(hid_st.at[par], hid_ref.at[par], hid_sem.at[par]).wait()

    @pl.loop(0, n_unit)
    def _(u):
        pltpu.make_async_copy(hbuf.at[u], saved_ref.at[u], save_sem.at[u]).wait()

    @pl.when(last)
    def _():
        @pl.loop(0, num_micro)
        def _(m):
            pltpu.make_async_copy(fbuf.at[m], hfin_ref.at[m], fin_c.at[m]).wait()
            remote(fbuf.at[m], fbuf.at[m], fin_a.at[m], fin_sem.at[m], n_stage - 2).wait_send()
            remote(fbuf.at[m], fbuf.at[m], fin_b.at[m], fin_sem.at[m], 1).wait_send()

    @pl.when(jnp.logical_not(last))
    def _():
        @pl.loop(0, num_micro)
        def _(m):
            remote(fbuf.at[m], fbuf.at[m], fin_a.at[m], fin_sem.at[m], right).wait_recv()

            @pl.when(me == 1)
            def _():
                remote(fbuf.at[m], fbuf.at[m], fin_a.at[m], fin_sem.at[m], 0).start()

            pltpu.make_async_copy(fbuf.at[m], hfin_ref.at[m], fin_c.at[m]).start()
            emit_norm(m)

        @pl.loop(0, num_micro)
        def _(m):
            pltpu.make_async_copy(fbuf.at[m], hfin_ref.at[m], fin_c.at[m]).wait()
            pltpu.make_async_copy(hbuf.at[m], n_ref.at[m], save_sem.at[m]).wait()

    @pl.when(me == 1)
    def _():
        @pl.loop(0, num_micro)
        def _(m):
            remote(fbuf.at[m], fbuf.at[m], fin_a.at[m], fin_sem.at[m], 0).wait_send()


def run_forward(x_embed, gains, w1, w2, w_head, n_tile, n_stage):
    num_micro, tokens, d_model = x_embed.shape
    d_ff = w1.shape[2]
    bf, f32 = jnp.bfloat16, jnp.float32
    n_unit = 2 * num_micro
    tile = w_head.shape[0] // n_tile
    last_rows = sub_tiles(tile)[-1][1]
    dma = pltpu.SemaphoreType.DMA
    return pl.pallas_call(
        functools.partial(fwd_kernel, n_stage, num_micro),
        name="stack_fwd",
        out_shape=(jax.ShapeDtypeStruct((n_unit, d_model, tokens), bf), jax.ShapeDtypeStruct((n_unit, d_ff, tokens), f32),
                   jax.ShapeDtypeStruct((n_unit, d_ff, tokens), bf), jax.ShapeDtypeStruct((num_micro, d_model, tokens), bf),
                   jax.ShapeDtypeStruct((num_micro, d_model, tokens), bf), jax.ShapeDtypeStruct((n_tile, d_model, tile), bf)),
        in_specs=[ANY, VMEM, VMEM, VMEM, ANY],
        out_specs=(ANY, ANY, ANY, ANY, ANY, ANY),
        scratch_shapes=[
            pltpu.VMEM((d_ff, d_model), bf), pltpu.VMEM((d_model, d_ff), bf),
            pltpu.VMEM((n_unit, d_model, tokens), bf), pltpu.VMEM((4, d_model, tokens), bf), pltpu.VMEM((num_micro, d_model, tokens), bf),
            pltpu.VMEM((2, d_ff, tokens), f32), pltpu.VMEM((2, d_ff, tokens), bf),
            pltpu.VMEM((SUB, d_model), bf), pltpu.VMEM((d_model, SUB), bf), pltpu.VMEM((last_rows, d_model), bf), pltpu.VMEM((d_model, last_rows), bf),
            dma((n_unit,)), dma((4,)), dma((n_unit,)), dma((2,)), dma((2,)), dma((num_micro,)), dma((num_micro,)), dma((num_micro,)), dma((num_micro,)),
            dma((2,)), dma((2,)),
        ],
        compiler_params=pltpu.CompilerParams(collective_id=0, has_side_effects=True, vmem_limit_bytes=VMEM_MAX),
        cost_estimate=pl.CostEstimate(flops=4 * n_unit * tokens * d_model * d_ff, bytes_accessed=7 * n_unit * d_ff * tokens, transcendentals=0),
    )(x_embed, gains, w1, w2, w_head)


def sub_tiles(tile):
    n_sub = tile // SUB
    return [(k * SUB, SUB if k + 1 < n_sub else tile - k * SUB) for k in range(n_sub)]


def label_group(lab):
    return jnp.where(lax.broadcasted_iota(jnp.int32, (8, lab.shape[1]), 0) == (lab & 7), lab >> 3, -1)


def logits_kernel(tile, n_all, lab_ref, w_ref, e_ref, mrun_ref, stat_ref, z0, z1, run):
    i = pl.program_id(0)
    num_micro = pl.num_programs(0)
    vocab, tokens = e_ref.shape[1], e_ref.shape[2]
    subs = sub_tiles(tile)
    n_sub, n_tile = len(subs), vocab // tile
    zbuf = (z0, z1)
    piece = 256
    low = jnp.full((8, tokens), -jnp.inf, jnp.float32)

    def rows_at(t, off, size):
        return pl.ds(pl.multiple_of(t * tile + off, 16), size)

    def dot_part(dst, t, off, size, base, n, group, top, hit):
        z = nn(w_ref[rows_at(t, off, size), :], n)
        dst[off - base:off - base + size, :] = z
        for g in range(size // 8):
            zg = z[g * 8:g * 8 + 8, :]
            top = jnp.maximum(top, zg)
            hit = jnp.where(group == t * (tile // 8) + (off // 8 + g), zg, hit)
        return top, hit

    def exp_part(src, t, base, lo, hi, m16, s8):
        for r in range(lo, hi, 16):
            e = jnp.exp(src[r:r + 16, :] - m16)
            e_ref[0, rows_at(t, base + r, 16), :] = e.astype(jnp.bfloat16)
            s8 = s8 + (e[0:8, :] + e[8:16, :])
        return s8

    def pieces(size):
        n_piece = size // piece
        return [(q * piece, piece if q + 1 < n_piece else size - q * piece) for q in range(n_piece)]

    def first_dot(m):
        n, group, top, hit = n_all[m], label_group(lab_ref[m]), low, jnp.zeros((8, tokens), jnp.float32)
        return n, group, top, hit

    def joint(kn, tn, n, group, top, hit, kc, tc, m, s8):
        m16 = jnp.broadcast_to(m, (16, tokens))
        base_n, size_n = subs[kn]
        base_c, size_c = subs[kc]
        parts = pieces(size_n)
        cut = -(-size_c // (16 * len(parts))) * 16
        for q, (off, size) in enumerate(parts):
            top, hit = dot_part(zbuf[kn % 2], tn, base_n + off, size, base_n, n, group, top, hit)
            s8 = exp_part(zbuf[kc % 2], tc, base_c, min(q * cut, size_c), min((q + 1) * cut, size_c), m16, s8)
        return top, hit, s8

    @pl.when(i == 0)
    def _():
        n, group, top, hit = first_dot(0)
        for off, size in pieces(subs[0][1]):
            top, hit = dot_part(z0, 0, off, size, 0, n, group, top, hit)
        run[0:8, :] = top
        run[8:16, :] = hit

    n = n_all[i]
    group = label_group(lab_ref[i])

    def step(kn, tn, kc, tc, carry):
        m, s8, hit = carry
        top, hit, s8 = joint(kn, tn, n, group, low, hit, kc, tc, m, s8)
        m_new = jnp.maximum(m, jnp.max(top, axis=0, keepdims=True))
        mrun_ref[0, pl.ds(tn * n_sub + kn, 1), :] = m_new
        return m_new, s8 * jnp.exp(m - m_new), hit

    m = jnp.max(run[0:8, :], axis=0, keepdims=True)
    mrun_ref[0, 0:1, :] = m
    carry = (m, jnp.zeros((8, tokens), jnp.float32), run[8:16, :])

    def body(t, carry):
        for k in range(n_sub):
            carry = step((k + 1) % n_sub, t + (k + 1) // n_sub, k, t, carry)
        return carry

    carry = lax.fori_loop(0, n_tile - 1, body, carry)
    for k in range(n_sub - 1):
        carry = step(k + 1, n_tile - 1, k, n_tile - 1, carry)
    m, s8, hit = carry
    n2, group2, top2, hit2 = first_dot(jnp.minimum(i + 1, num_micro - 1))
    top2, hit2, s8 = joint(0, 0, n2, group2, top2, hit2, n_sub - 1, n_tile - 1, m, s8)
    run[0:8, :] = top2
    run[8:16, :] = hit2
    stat_ref[0, 0:1, :] = m
    stat_ref[0, 1:2, :] = jnp.sum(s8, axis=0, keepdims=True)
    stat_ref[0, 2:3, :] = jnp.sum(hit, axis=0, keepdims=True)


def d_logits(e_tile, fac_row, lab, off, inv):
    hit = lax.broadcasted_iota(jnp.int32, e_tile.shape, 0) == lab - off
    return (e_tile.astype(jnp.float32) * fac_row - jnp.where(hit, inv, 0.0)).astype(jnp.bfloat16)


def dnorm_kernel(inv, e_ref, fac_ref, lab_ref, wt_ref, dn_ref):
    j = pl.program_id(1)
    tile = e_ref.shape[1]
    subs = sub_tiles(tile)
    lab = lab_ref[0] - j * tile
    total = None
    for k, (off, size) in enumerate(subs):
        d = d_logits(e_ref[0, off:off + size, :], fac_ref[0, pl.ds(j * len(subs) + k, 1), :], lab, off, inv)
        part = nn(wt_ref[j, :, off:off + size], d)
        total = part if total is None else total + part

    @pl.when(j == 0)
    def _():
        dn_ref[0] = total

    @pl.when(j > 0)
    def _():
        dn_ref[0] += total


def dhead_kernel(inv, e_ref, fac_ref, lab_ref, n_ref, out_ref, acc):
    j, i = pl.program_id(0), pl.program_id(1)
    tile = e_ref.shape[1]
    subs = sub_tiles(tile)
    per = e_ref.shape[0]

    @pl.when(i == 0)
    def _():
        acc[...] = jnp.zeros_like(acc)

    for k, (off, size) in enumerate(subs):
        total = None
        for b in range(per):
            d = d_logits(e_ref[b, off:off + size, :], fac_ref[b, pl.ds(j * len(subs) + k, 1), :], lab_ref[b] - j * tile, off, inv)
            part = nt(d, n_ref[b])
            total = part if total is None else total + part
        acc[off:off + size, :] += total

    @pl.when(i == pl.num_programs(1) - 1)
    def _():
        out_ref[...] = acc[...].astype(jnp.bfloat16)


def run_head(h_fin, n_t, wt, labels, w_head, stage_id, n_stage):
    num_micro, d_model, tokens = h_fin.shape
    vocab = w_head.shape[0]
    n_tile, tile = wt.shape[0], wt.shape[2]
    n_row = 16
    bf, f32 = jnp.bfloat16, jnp.float32
    inv = 1.0 / (num_micro * tokens)
    lab = (labels - stage_id * vocab).reshape(num_micro, 1, tokens)
    params = pltpu.CompilerParams(vmem_limit_bytes=VMEM_MAX)
    cost = pl.CostEstimate(flops=2 * num_micro * tokens * d_model * vocab, bytes_accessed=2 * num_micro * tokens * vocab, transcendentals=0)

    def micro(shape):
        return pl.BlockSpec(shape, lambda i: (i, 0, 0))

    def micro2(shape):
        return pl.BlockSpec(shape, lambda i, j: (i, 0, 0))

    z_rows = tile - (tile // SUB - 1) * SUB
    e, m_run, stat = pl.pallas_call(
        functools.partial(logits_kernel, tile), name="head_logits",
        grid=(num_micro,),
        out_shape=(jax.ShapeDtypeStruct((num_micro, vocab, tokens), bf), jax.ShapeDtypeStruct((num_micro, n_row, tokens), f32),
                   jax.ShapeDtypeStruct((num_micro, 8, tokens), f32)),
        in_specs=[VMEM, VMEM, VMEM],
        out_specs=(micro((1, vocab, tokens)), micro((1, n_row, tokens)), micro((1, 8, tokens))),
        scratch_shapes=[pltpu.VMEM((z_rows, tokens), f32), pltpu.VMEM((z_rows, tokens), f32), pltpu.VMEM((16, tokens), f32)],
        compiler_params=params, cost_estimate=cost,
    )(n_t, lab, w_head)

    stats = lax.all_gather(stat[:, :3, :], 'pp')
    m_all, s_all = stats[:, :, 0], stats[:, :, 1]
    m_top = jnp.max(m_all, axis=0)
    s_top = jnp.sum(s_all * jnp.exp(m_all - m_top), axis=0)
    loss = jnp.sum(m_top + jnp.log(s_top) - jnp.sum(stats[:, :, 2], axis=0)) * inv
    fac = jnp.exp(m_run - m_top[:, None, :]) * (inv / s_top)[:, None, :]

    dn = pl.pallas_call(
        functools.partial(dnorm_kernel, inv), name="head_dnorm",
        grid=(num_micro, n_tile),
        out_shape=jax.ShapeDtypeStruct((num_micro, d_model, tokens), f32),
        in_specs=[pl.BlockSpec((1, tile, tokens), lambda i, j: (i, j, 0)), micro2((1, n_row, tokens)), micro2((1, 1, tokens)), VMEM],
        out_specs=micro2((1, d_model, tokens)),
        compiler_params=params, cost_estimate=cost,
    )(e, fac, lab, wt)

    per = 2
    head_grad = pl.pallas_call(
        functools.partial(dhead_kernel, inv), name="head_dweight",
        grid=(n_tile, num_micro // per),
        out_shape=jax.ShapeDtypeStruct((vocab, d_model), bf),
        in_specs=[pl.BlockSpec((per, tile, tokens), lambda j, i: (i, j, 0)), pl.BlockSpec((per, n_row, tokens), lambda j, i: (i, 0, 0)),
                  pl.BlockSpec((per, 1, tokens), lambda j, i: (i, 0, 0)), pl.BlockSpec((per, d_model, tokens), lambda j, i: (i, 0, 0))],
        out_specs=pl.BlockSpec((tile, d_model), lambda j, i: (j, 0)),
        scratch_shapes=[pltpu.VMEM((tile, d_model), f32)],
        compiler_params=params, cost_estimate=cost,
    )(e, fac, lab, n_t)

    dn_own = lax.psum_scatter(dn, 'pp', scatter_dimension=0, tiled=True)
    per_stage = num_micro // n_stage
    h_own = lax.dynamic_slice_in_dim(h_fin, stage_id * per_stage, per_stage, 0).astype(f32)
    r_own = lax.rsqrt(jnp.mean(h_own * h_own, axis=1, keepdims=True) + NORM_EPS)
    n_own = h_own * r_own
    d_fin = r_own * (dn_own - n_own * jnp.mean(dn_own * n_own, axis=1, keepdims=True))
    return loss, head_grad, d_fin.astype(bf)


def bwd_kernel(n_stage, num_micro, dfin_ref, saved_ref, slope_ref, hid_ref, g_ref, w1_ref, w2_ref, dw1_ref, dw2_ref, dg_ref, dx_ref,
               dbuf, obuf, xbuf, h_in, slope_in, hid_in, dpre, acc1, acc2, accg, st1, st2, gb, hrb, dyb, yb,
               in_sem, push_sem, out_sem, x_sem, xr_sem, h_sem, slope_sem, hid_sem, w_sem):
    me = lax.axis_index("pp")
    left = lax.rem(me + n_stage - 1, n_stage)
    first, last = me == 0, me == n_stage - 1
    n_unit = 2 * num_micro
    per = num_micro // n_stage
    d_model, d_ff = w1_ref.shape[1:]
    step = 512
    group_barrier(me, n_stage)

    def fetch(w):
        u, par = n_unit - 1 - w, lax.rem(w, 2)
        return (pltpu.make_async_copy(saved_ref.at[u], h_in.at[par], h_sem.at[par]),
                pltpu.make_async_copy(slope_ref.at[u], slope_in.at[par], slope_sem.at[par]),
                pltpu.make_async_copy(hid_ref.at[u], hid_in.at[par], hid_sem.at[par]))

    for copy in fetch(0):
        copy.start()

    @pl.when(last)
    def _():
        for i in range(per):
            slot = num_micro - 1 - (per * (n_stage - 1) + i)
            pltpu.make_async_copy(dfin_ref.at[i], dbuf.at[slot], in_sem.at[slot]).start()

    @pl.when(jnp.logical_not(last))
    def _():
        for i in reversed(range(per)):
            slot = num_micro - 1 - (per * me + i)
            remote(dfin_ref.at[i], dbuf.at[slot], push_sem.at[i], in_sem.at[slot], n_stage - 1).start()

    @pl.loop(0, n_unit)
    def _(w):
        half = 1 - w // num_micro
        par = lax.rem(w, 2)
        is_local = last & (w < per)
        is_final = first & (half == 0)

        @pl.when(w + 1 < n_unit)
        def _():
            for copy in fetch(w + 1):
                copy.start()

        @pl.when(lax.rem(w, num_micro) == 0)
        def _():
            acc1[...] = jnp.zeros_like(acc1)
            acc2[...] = jnp.zeros_like(acc2)
            accg[...] = jnp.zeros_like(accg)
            gb[...] = jnp.broadcast_to(g_ref[half], gb.shape)

        @pl.when(is_local)
        def _():
            pltpu.make_async_copy(dfin_ref.at[0], dbuf.at[w], in_sem.at[w]).wait()

        @pl.when(jnp.logical_not(is_local))
        def _():
            remote(obuf.at[0], dbuf.at[w], out_sem.at[0], in_sem.at[w], left).wait_recv()

        for copy in fetch(w):
            copy.wait()

        d_in = dbuf[w]
        nxt = nn(w2_ref[half, 0:step, :], d_in)
        for k in range(d_ff // step):
            rows = pl.ds(k * step, step)
            cur = nxt
            if k + 1 < d_ff // step:
                nxt = nn(w2_ref[half, (k + 1) * step:(k + 2) * step, :], d_in)
            dpre[rows, :] = (cur * slope_in[par, rows, :]).astype(jnp.bfloat16)
        h = h_in[par].astype(jnp.float32)
        r = col_scale(h)
        r16 = jnp.broadcast_to(r, (16, r.shape[1]))
        for q in range(0, d_model, 16):
            hr = h_in[par, q:q + 16, :].astype(jnp.float32) * r16
            hrb[q:q + 16, :] = hr
            yb[q:q + 16, :] = (hr * gb[q:q + 16, :]).astype(jnp.bfloat16)
        dyb[...] = nn(w1_ref[half], dpre[...])
        dots = jnp.zeros_like(r16)
        for q in range(0, d_model, 16):
            prod = dyb[q:q + 16, :] * hrb[q:q + 16, :]
            accg[q:q + 16, :] += prod
            dots = dots + prod * gb[q:q + 16, :]
        mean16 = jnp.broadcast_to(jnp.sum(dots, axis=0, keepdims=True) * (1.0 / d_model), r16.shape)
        for q in range(0, d_model, 16):
            dyb[q:q + 16, :] = dbuf[w, q:q + 16, :].astype(jnp.float32) + r16 * (dyb[q:q + 16, :] * gb[q:q + 16, :] - hrb[q:q + 16, :] * mean16)

        @pl.when(is_final)
        def _():
            q = w - num_micro
            slot = lax.rem(q, 4)
            m = num_micro - 1 - q
            owner, i = m // per, lax.rem(m, per)

            @pl.when(q >= 4)
            def _():
                remote(xbuf.at[slot], dx_ref.at[0], x_sem.at[slot], xr_sem.at[0], left).wait_send()

            xbuf[slot] = dyb[...]

            @pl.when(owner == 0)
            def _():
                pltpu.make_async_copy(xbuf.at[slot], dx_ref.at[i], x_sem.at[slot]).start()

            @pl.when(owner > 0)
            def _():
                remote(xbuf.at[slot], dx_ref.at[i], x_sem.at[slot], xr_sem.at[i], jnp.maximum(owner, 1)).start()

        @pl.when(jnp.logical_not(is_final))
        def _():
            slot = lax.rem(w, 4)

            @pl.when(w >= 4)
            def _():
                remote(obuf.at[slot], dbuf.at[w], out_sem.at[slot], in_sem.at[w], left).wait_send()

            obuf[slot] = dyb[...].astype(jnp.bfloat16)
            dst = w + jnp.where(first, num_micro, 0)
            remote(obuf.at[slot], dbuf.at[dst], out_sem.at[slot], in_sem.at[dst], left).start()

        y = yb[...]
        for k in range(d_ff // step):
            rows = pl.ds(k * step, step)
            acc2[rows, :] += nt(hid_in[par, rows, :], d_in)
            acc1[:, rows] += nt(y, dpre[rows, :])

        @pl.when(lax.rem(w, num_micro) == num_micro - 1)
        def _():
            @pl.when(half == 0)
            def _():
                pltpu.make_async_copy(st1, dw1_ref.at[1], w_sem.at[0]).wait()
                pltpu.make_async_copy(st2, dw2_ref.at[1], w_sem.at[1]).wait()

            st1[...] = acc1[...].astype(jnp.bfloat16)
            st2[...] = acc2[...].astype(jnp.bfloat16)
            dg_ref[half] = jnp.sum(accg[...], axis=1, keepdims=True)
            pltpu.make_async_copy(st1, dw1_ref.at[half], w_sem.at[0]).start()
            pltpu.make_async_copy(st2, dw2_ref.at[half], w_sem.at[1]).start()

    pltpu.make_async_copy(st1, dw1_ref.at[0], w_sem.at[0]).wait()
    pltpu.make_async_copy(st2, dw2_ref.at[0], w_sem.at[1]).wait()
    for slot in range(4):
        remote(obuf.at[slot], dbuf.at[0], out_sem.at[slot], in_sem.at[0], left).wait_send()

    @pl.when(jnp.logical_not(last))
    def _():
        for i in range(per):
            remote(dfin_ref.at[i], dbuf.at[0], push_sem.at[i], in_sem.at[0], n_stage - 1).wait_send()

    @pl.when(first)
    def _():
        remote(xbuf.at[0], dx_ref.at[0], x_sem.at[0], xr_sem.at[0], left).wait_send()
        for slot in range(1, 4):
            pltpu.make_async_copy(xbuf.at[slot], dx_ref.at[0], x_sem.at[slot]).wait()

    @pl.when(jnp.logical_not(first))
    def _():
        for i in range(per):
            remote(xbuf.at[0], dx_ref.at[i], x_sem.at[0], xr_sem.at[i], left).wait_recv()


def run_backward(d_fin, saved, slope, hid, gains, w1, w2, n_stage):
    n_unit, d_model, tokens = saved.shape
    num_micro = n_unit // 2
    d_ff = w1.shape[2]
    per = num_micro // n_stage
    bf, f32 = jnp.bfloat16, jnp.float32
    dma = pltpu.SemaphoreType.DMA
    return pl.pallas_call(
        functools.partial(bwd_kernel, n_stage, num_micro),
        name="stack_bwd",
        out_shape=(jax.ShapeDtypeStruct(w1.shape, bf), jax.ShapeDtypeStruct(w2.shape, bf), jax.ShapeDtypeStruct((2, d_model, 1), f32),
                   jax.ShapeDtypeStruct((per, d_model, tokens), f32)),
        in_specs=[ANY, ANY, ANY, ANY, VMEM, VMEM, VMEM],
        out_specs=(ANY, ANY, VMEM, ANY),
        scratch_shapes=[
            pltpu.VMEM((n_unit, d_model, tokens), bf), pltpu.VMEM((4, d_model, tokens), bf), pltpu.VMEM((4, d_model, tokens), f32),
            pltpu.VMEM((2, d_model, tokens), bf), pltpu.VMEM((2, d_ff, tokens), f32), pltpu.VMEM((2, d_ff, tokens), bf),
            pltpu.VMEM((d_ff, tokens), bf), pltpu.VMEM((d_model, d_ff), f32), pltpu.VMEM((d_ff, d_model), f32), pltpu.VMEM((d_model, tokens), f32),
            pltpu.VMEM((d_model, d_ff), bf), pltpu.VMEM((d_ff, d_model), bf),
            pltpu.VMEM((d_model, tokens), f32), pltpu.VMEM((d_model, tokens), f32), pltpu.VMEM((d_model, tokens), f32), pltpu.VMEM((d_model, tokens), bf),
            dma((n_unit,)), dma((per,)), dma((4,)), dma((4,)), dma((per,)), dma((2,)), dma((2,)), dma((2,)), dma((2,)),
        ],
        compiler_params=pltpu.CompilerParams(collective_id=1, has_side_effects=True, vmem_limit_bytes=VMEM_MAX),
        cost_estimate=pl.CostEstimate(flops=8 * n_unit * tokens * d_model * d_ff, bytes_accessed=7 * n_unit * d_ff * tokens, transcendentals=0),
    )(d_fin, saved, slope, hid, gains, w1, w2)


def solution(mesh):
    n_stage = mesh.shape['pp']

    def local_step(x_embed, labels, norm_gain, w_up, w_down, w_head):
        stage_id = lax.axis_index('pp')
        gains = jnp.swapaxes(norm_gain[0], 1, 2)
        w1, w2 = w_up[0, :, 0], w_down[0, :, 0]
        saved, slope, hid, h_fin, n_t, wt = run_forward(x_embed, gains, w1, w2, w_head, 3, n_stage)
        loss, head_grad, d_fin = run_head(h_fin, n_t, wt, labels, w_head, stage_id, n_stage)
        dw1, dw2, dg, dx = run_backward(d_fin, saved, slope, hid, gains, w1, w2, n_stage)
        return (loss.reshape(1), jnp.swapaxes(dx, 1, 2), jnp.swapaxes(dg, 1, 2)[None], dw1[None, :, None], dw2[None, :, None], head_grad)

    part_spec = P('dp')
    stage_spec = P('pp')
    out_spec = P(('dp', 'pp'))
    return jax.shard_map(local_step, mesh=mesh, in_specs=(part_spec, part_spec, stage_spec, stage_spec, stage_spec, stage_spec), out_specs=(part_spec, out_spec, out_spec, out_spec, out_spec, out_spec), check_vma=False)
```

```python
import functools

import jax
import jax.numpy as jnp
from jax import lax
from jax.experimental import pallas as pl
from jax.experimental.pallas import tpu as pltpu
from jax.sharding import PartitionSpec as P

NORM_EPS = 1e-6
VMEM_MAX = 67_000_000
GELU_A = 0.7978845608028654
GELU_B = GELU_A * 0.044715
SUB = 1024
RANGE = 40.0

ANY = pl.BlockSpec(memory_space=pl.ANY)
VMEM = pl.BlockSpec(memory_space=pltpu.VMEM)


def nn(lhs, rhs):
    return lax.dot_general(lhs, rhs, (((1,), (0,)), ((), ())), preferred_element_type=jnp.float32)


def nt(lhs, rhs):
    return lax.dot_general(lhs, rhs, (((1,), (1,)), ((), ())), preferred_element_type=jnp.float32)


def col_scale(h_f32):
    return lax.rsqrt(jnp.mean(h_f32 * h_f32, axis=0, keepdims=True) + NORM_EPS)


def gelu_pair(x):
    x2 = x * x
    th = jnp.tanh(x * (GELU_A + GELU_B * x2))
    hx = 0.5 * x
    slope = 0.5 + 0.5 * th + hx * (1.0 - th * th) * (GELU_A + (3.0 * GELU_B) * x2)
    return hx + hx * th, slope


def group_barrier(me, n_stage):
    sem = pltpu.get_barrier_semaphore()
    for step in range(1, n_stage):
        pl.semaphore_signal(sem, inc=1, device_id={"pp": lax.rem(me + step, n_stage)}, device_id_type=pl.DeviceIdType.MESH)
    pl.semaphore_wait(sem, n_stage - 1)


def remote(src, dst, send_sem, recv_sem, dev):
    return pltpu.make_async_remote_copy(src_ref=src, dst_ref=dst, send_sem=send_sem, recv_sem=recv_sem, device_id={"pp": dev}, device_id_type=pl.DeviceIdType.MESH)


def fwd_kernel(n_stage, num_micro, x_ref, g_ref, w1_ref, w2_ref, wh_ref, saved_ref, slope_ref, hid_ref, hfin_ref, n_ref, wht_ref,
               w1t, w2t, hbuf, obuf, fbuf, slope_st, hid_st, wh_in, wh_out, wh_last, wht_last, in_sem, out_sem, save_sem, slope_sem, hid_sem, fin_sem, fin_a, fin_b, fin_c, whi_sem, who_sem):
    me = lax.axis_index("pp")
    right = lax.rem(me + 1, n_stage)
    first, last = me == 0, me == n_stage - 1
    n_unit = 2 * num_micro
    d_ff = w1_ref.shape[2]
    n_tile, tile = wht_ref.shape[0], wht_ref.shape[2]
    subs = sub_tiles(tile)
    group_barrier(me, n_stage)

    def emit_norm(m):
        hf = fbuf[m].astype(jnp.float32)
        hbuf[m] = (hf * col_scale(hf)).astype(jnp.bfloat16)
        pltpu.make_async_copy(hbuf.at[m], n_ref.at[m], save_sem.at[m]).start()

    def head_copies(t, k):
        off, size = subs[k]
        last_sub = k + 1 == len(subs)
        src, dst = (wh_last, wht_last) if last_sub else (wh_in, wh_out)
        rows = pl.ds(pl.multiple_of(t * tile + off, 16), size)
        return (src, dst, lambda: pltpu.make_async_copy(wh_ref.at[rows, :], src, whi_sem.at[int(last_sub)]),
                lambda: pltpu.make_async_copy(dst, wht_ref.at[t, :, off:off + size], who_sem.at[int(last_sub)]))

    @pl.when(first)
    def _():
        @pl.loop(0, num_micro)
        def _(m):
            pltpu.make_async_copy(x_ref.at[m], hbuf.at[m], in_sem.at[m]).start()

    @pl.loop(0, n_unit)
    def _(u):
        half = u // num_micro

        @pl.when(lax.rem(u, num_micro) == 0)
        def _():
            w1t[...] = w1_ref[half].T
            w2t[...] = w2_ref[half].T

        m = lax.rem(u, num_micro)
        from_x = first & (half == 0)
        is_final = last & (half == 1)
        par = lax.rem(u, 2)

        @pl.when(from_x)
        def _():
            pltpu.make_async_copy(x_ref.at[m], hbuf.at[u], in_sem.at[u]).wait()
            hbuf[u] = hbuf[u].T

        @pl.when(jnp.logical_not(from_x))
        def _():
            remote(obuf.at[0], hbuf.at[u], out_sem.at[0], in_sem.at[u], right).wait_recv()

        pltpu.make_async_copy(hbuf.at[u], saved_ref.at[u], save_sem.at[u]).start()

        @pl.when(u >= 2)
        def _():
            pltpu.make_async_copy(slope_st.at[par], slope_ref.at[u - 2], slope_sem.at[par]).wait()
            pltpu.make_async_copy(hid_st.at[par], hid_ref.at[u - 2], hid_sem.at[par]).wait()

        h = hbuf[u].astype(jnp.float32)
        y = (h * col_scale(h) * g_ref[half]).astype(jnp.bfloat16)
        step = 512
        pre = nn(w1t[0:step, :], y)
        for k in range(d_ff // step):
            rows = pl.ds(k * step, step)
            cur = pre
            if k + 1 < d_ff // step:
                pre = nn(w1t[(k + 1) * step:(k + 2) * step, :], y)
            hid, slope = gelu_pair(cur)
            hid_st[par, rows, :] = hid.astype(jnp.bfloat16)
            slope_st[par, rows, :] = slope
        out = (h + nn(w2t[...], hid_st[par])).astype(jnp.bfloat16)
        pltpu.make_async_copy(slope_st.at[par], slope_ref.at[u], slope_sem.at[par]).start()
        pltpu.make_async_copy(hid_st.at[par], hid_ref.at[u], hid_sem.at[par]).start()

        @pl.when(is_final)
        def _():
            fbuf[m] = out
            pltpu.make_async_copy(fbuf.at[m], hfin_ref.at[m], fin_c.at[m]).start()
            remote(fbuf.at[m], fbuf.at[m], fin_a.at[m], fin_sem.at[m], n_stage - 2).start()
            remote(fbuf.at[m], fbuf.at[m], fin_b.at[m], fin_sem.at[m], 1).start()
            pltpu.make_async_copy(hbuf.at[m], saved_ref.at[m], save_sem.at[m]).wait()
            emit_norm(m)

        @pl.when(jnp.logical_not(is_final))
        def _():
            slot = lax.rem(u, 4)

            @pl.when(u >= 4)
            def _():
                remote(obuf.at[slot], hbuf.at[u], out_sem.at[slot], in_sem.at[u], right).wait_send()

            obuf[slot] = out
            dst = u + jnp.where(last, num_micro, 0)
            remote(obuf.at[slot], hbuf.at[dst], out_sem.at[slot], in_sem.at[dst], right).start()

        for k in range(len(subs)):
            @pl.when((lax.rem(u, 2 * len(subs)) == 2 * k) & (u // (2 * len(subs)) < n_tile))
            def _(k=k):
                head_copies(u // (2 * len(subs)), k)[2]().start()

            @pl.when((lax.rem(u, 2 * len(subs)) == 2 * k + 1) & (u // (2 * len(subs)) < n_tile))
            def _(k=k):
                t = u // (2 * len(subs))
                src, dst, copy_in, copy_out = head_copies(t, k)
                copy_in().wait()
                dst[...] = src[...].T
                copy = copy_out()
                copy.start()
                copy.wait()

    for slot in range(4):
        remote(obuf.at[slot], hbuf.at[0], out_sem.at[slot], in_sem.at[0], right).wait_send()
    for par in range(2):
        pltpu.make_async_copy(slope_st.at[par], slope_ref.at[par], slope_sem.at[par]).wait()
        pltpu.make_async_copy(hid_st.at[par], hid_ref.at[par], hid_sem.at[par]).wait()

    @pl.loop(0, n_unit)
    def _(u):
        pltpu.make_async_copy(hbuf.at[u], saved_ref.at[u], save_sem.at[u]).wait()

    @pl.when(last)
    def _():
        @pl.loop(0, num_micro)
        def _(m):
            pltpu.make_async_copy(fbuf.at[m], hfin_ref.at[m], fin_c.at[m]).wait()
            remote(fbuf.at[m], fbuf.at[m], fin_a.at[m], fin_sem.at[m], n_stage - 2).wait_send()
            remote(fbuf.at[m], fbuf.at[m], fin_b.at[m], fin_sem.at[m], 1).wait_send()

    @pl.when(jnp.logical_not(last))
    def _():
        @pl.loop(0, num_micro)
        def _(m):
            remote(fbuf.at[m], fbuf.at[m], fin_a.at[m], fin_sem.at[m], right).wait_recv()

            @pl.when(me == 1)
            def _():
                remote(fbuf.at[m], fbuf.at[m], fin_a.at[m], fin_sem.at[m], 0).start()

            pltpu.make_async_copy(fbuf.at[m], hfin_ref.at[m], fin_c.at[m]).start()
            emit_norm(m)

        @pl.loop(0, num_micro)
        def _(m):
            pltpu.make_async_copy(fbuf.at[m], hfin_ref.at[m], fin_c.at[m]).wait()
            pltpu.make_async_copy(hbuf.at[m], n_ref.at[m], save_sem.at[m]).wait()

    @pl.when(me == 1)
    def _():
        @pl.loop(0, num_micro)
        def _(m):
            remote(fbuf.at[m], fbuf.at[m], fin_a.at[m], fin_sem.at[m], 0).wait_send()


def run_forward(x_embed, gains, w1, w2, w_head, n_tile, n_stage):
    num_micro, tokens, d_model = x_embed.shape
    d_ff = w1.shape[2]
    bf, f32 = jnp.bfloat16, jnp.float32
    n_unit = 2 * num_micro
    tile = w_head.shape[0] // n_tile
    last_rows = sub_tiles(tile)[-1][1]
    dma = pltpu.SemaphoreType.DMA
    return pl.pallas_call(
        functools.partial(fwd_kernel, n_stage, num_micro),
        name="stack_fwd",
        out_shape=(jax.ShapeDtypeStruct((n_unit, d_model, tokens), bf), jax.ShapeDtypeStruct((n_unit, d_ff, tokens), f32),
                   jax.ShapeDtypeStruct((n_unit, d_ff, tokens), bf), jax.ShapeDtypeStruct((num_micro, d_model, tokens), bf),
                   jax.ShapeDtypeStruct((num_micro, d_model, tokens), bf), jax.ShapeDtypeStruct((n_tile, d_model, tile), bf)),
        in_specs=[ANY, VMEM, VMEM, VMEM, ANY],
        out_specs=(ANY, ANY, ANY, ANY, ANY, ANY),
        scratch_shapes=[
            pltpu.VMEM((d_ff, d_model), bf), pltpu.VMEM((d_model, d_ff), bf),
            pltpu.VMEM((n_unit, d_model, tokens), bf), pltpu.VMEM((4, d_model, tokens), bf), pltpu.VMEM((num_micro, d_model, tokens), bf),
            pltpu.VMEM((2, d_ff, tokens), f32), pltpu.VMEM((2, d_ff, tokens), bf),
            pltpu.VMEM((SUB, d_model), bf), pltpu.VMEM((d_model, SUB), bf), pltpu.VMEM((last_rows, d_model), bf), pltpu.VMEM((d_model, last_rows), bf),
            dma((n_unit,)), dma((4,)), dma((n_unit,)), dma((2,)), dma((2,)), dma((num_micro,)), dma((num_micro,)), dma((num_micro,)), dma((num_micro,)),
            dma((2,)), dma((2,)),
        ],
        compiler_params=pltpu.CompilerParams(collective_id=0, has_side_effects=True, vmem_limit_bytes=VMEM_MAX),
        cost_estimate=pl.CostEstimate(flops=4 * n_unit * tokens * d_model * d_ff, bytes_accessed=7 * n_unit * d_ff * tokens, transcendentals=0),
    )(x_embed, gains, w1, w2, w_head)


def sub_tiles(tile):
    n_sub = tile // SUB
    return [(k * SUB, SUB if k + 1 < n_sub else tile - k * SUB) for k in range(n_sub)]


def logits_kernel(tile, n_ref, lab_ref, w_ref, e_ref, mrun_ref, stat_ref, used, s_buf):
    vocab, tokens = e_ref.shape[1], e_ref.shape[2]
    n_tile = vocab // tile
    piece, small = 256, 32
    n = n_ref[0]
    lab = lab_ref[0]
    group = jnp.where(lax.broadcasted_iota(jnp.int32, (8, tokens), 0) == (lab & 7), lab >> 3, -1)

    def rows_at(t, off, size):
        return pl.ds(pl.multiple_of(t * tile + off, 16), size)

    def body(t, carry):
        m_run, s_run, hit = carry
        m_use = jnp.where(t == 0, 0.0, m_run)
        m8 = jnp.broadcast_to(m_use, (8, tokens))
        top = jnp.full((8, tokens), -jnp.inf, jnp.float32)
        s8 = jnp.zeros((8, tokens), jnp.float32)
        local = group - t * (tile // 8)
        n_piece = tile // piece
        for q in range(n_piece):
            off = q * piece
            size = piece if q + 1 < n_piece else tile - off
            z = nn(w_ref[rows_at(t, off, size), :], n)
            for r in range(0, size, 16):
                e = []
                for g in range(2):
                    zg = z[r + 8 * g:r + 8 * g + 8, :]
                    top = jnp.maximum(top, zg)
                    hit = jnp.where(local == (off + r) // 8 + g, zg, hit)
                    e.append(jnp.exp(zg - m8))
                    s8 = s8 + e[g]
                e_ref[0, rows_at(t, off + r, 16), :] = jnp.concatenate(e, axis=0).astype(jnp.bfloat16)
        m_new = jnp.maximum(m_run, jnp.max(top, axis=0, keepdims=True))
        used[0:1, :] = m_use
        s_buf[...] = s8
        rise = jnp.max(m_new - m_use)
        fall = jnp.max(m_use - m_new)

        @pl.when((rise > RANGE) | (fall > RANGE))
        def _():
            used[0:1, :] = m_new
            s_buf[...] = jnp.zeros_like(s_buf)

            @pl.loop(0, tile // small)
            def _(q):
                e = jnp.exp(nn(w_ref[rows_at(t, q * small, small), :], n) - m_new)
                e_ref[0, rows_at(t, q * small, small), :] = e.astype(jnp.bfloat16)
                for r in range(0, small, 8):
                    s_buf[...] += e[r:r + 8, :]

        m_use = used[0:1, :]
        mrun_ref[0, pl.ds(t, 1), :] = m_use
        s_run = s_run * jnp.exp(m_run - m_new) + s_buf[...] * jnp.exp(m_use - m_new)
        return m_new, s_run, hit

    low = jnp.full((1, tokens), -jnp.inf, jnp.float32)
    zero = jnp.zeros((8, tokens), jnp.float32)
    m, s8, hit = lax.fori_loop(0, n_tile, body, (low, zero, zero))
    stat_ref[0, 0:1, :] = m
    stat_ref[0, 1:2, :] = jnp.sum(s8, axis=0, keepdims=True)
    stat_ref[0, 2:3, :] = jnp.sum(hit, axis=0, keepdims=True)


def d_logits(e_tile, fac_row, lab, off, inv):
    hit = lax.broadcasted_iota(jnp.int32, e_tile.shape, 0) == lab - off
    return (e_tile.astype(jnp.float32) * fac_row - jnp.where(hit, inv, 0.0)).astype(jnp.bfloat16)


def dnorm_kernel(inv, e_ref, fac_ref, lab_ref, wt_ref, dn_ref):
    j = pl.program_id(1)
    tile = e_ref.shape[1]
    subs = sub_tiles(tile)
    lab = lab_ref[0] - j * tile
    total = None
    for k, (off, size) in enumerate(subs):
        d = d_logits(e_ref[0, off:off + size, :], fac_ref[0, pl.ds(j, 1), :], lab, off, inv)
        part = nn(wt_ref[j, :, off:off + size], d)
        total = part if total is None else total + part

    @pl.when(j == 0)
    def _():
        dn_ref[0] = total

    @pl.when(j > 0)
    def _():
        dn_ref[0] += total


def dhead_kernel(inv, e_ref, fac_ref, lab_ref, n_ref, out_ref, acc):
    j, i = pl.program_id(0), pl.program_id(1)
    tile = e_ref.shape[1]
    subs = sub_tiles(tile)
    per = e_ref.shape[0]

    @pl.when(i == 0)
    def _():
        acc[...] = jnp.zeros_like(acc)

    for k, (off, size) in enumerate(subs):
        total = None
        for b in range(per):
            d = d_logits(e_ref[b, off:off + size, :], fac_ref[b, pl.ds(j, 1), :], lab_ref[b] - j * tile, off, inv)
            part = nt(d, n_ref[b])
            total = part if total is None else total + part
        acc[off:off + size, :] += total

    @pl.when(i == pl.num_programs(1) - 1)
    def _():
        out_ref[...] = acc[...].astype(jnp.bfloat16)


def run_head(h_fin, n_t, wt, labels, w_head, stage_id, n_stage):
    num_micro, d_model, tokens = h_fin.shape
    vocab = w_head.shape[0]
    n_tile, tile = wt.shape[0], wt.shape[2]
    n_row = 8
    bf, f32 = jnp.bfloat16, jnp.float32
    inv = 1.0 / (num_micro * tokens)
    lab = (labels - stage_id * vocab).reshape(num_micro, 1, tokens)
    params = pltpu.CompilerParams(vmem_limit_bytes=VMEM_MAX)
    cost = pl.CostEstimate(flops=2 * num_micro * tokens * d_model * vocab, bytes_accessed=2 * num_micro * tokens * vocab, transcendentals=0)

    def micro(shape):
        return pl.BlockSpec(shape, lambda i: (i, 0, 0))

    def micro2(shape):
        return pl.BlockSpec(shape, lambda i, j: (i, 0, 0))

    e, m_run, stat = pl.pallas_call(
        functools.partial(logits_kernel, tile), name="head_logits",
        grid=(num_micro,),
        out_shape=(jax.ShapeDtypeStruct((num_micro, vocab, tokens), bf), jax.ShapeDtypeStruct((num_micro, n_row, tokens), f32),
                   jax.ShapeDtypeStruct((num_micro, 8, tokens), f32)),
        in_specs=[micro((1, d_model, tokens)), micro((1, 1, tokens)), VMEM],
        out_specs=(micro((1, vocab, tokens)), micro((1, n_row, tokens)), micro((1, 8, tokens))),
        scratch_shapes=[pltpu.VMEM((8, tokens), f32), pltpu.VMEM((8, tokens), f32)],
        compiler_params=params, cost_estimate=cost,
    )(n_t, lab, w_head)

    stats = lax.all_gather(stat[:, :3, :], 'pp')
    m_all, s_all = stats[:, :, 0], stats[:, :, 1]
    m_top = jnp.max(m_all, axis=0)
    s_top = jnp.sum(s_all * jnp.exp(m_all - m_top), axis=0)
    loss = jnp.sum(m_top + jnp.log(s_top) - jnp.sum(stats[:, :, 2], axis=0)) * inv
    fac = jnp.exp(m_run[:, :n_tile] - m_top[:, None, :]) * (inv / s_top)[:, None, :]

    dn = pl.pallas_call(
        functools.partial(dnorm_kernel, inv), name="head_dnorm",
        grid=(num_micro, n_tile),
        out_shape=jax.ShapeDtypeStruct((num_micro, d_model, tokens), f32),
        in_specs=[pl.BlockSpec((1, tile, tokens), lambda i, j: (i, j, 0)), micro2((1, n_tile, tokens)), micro2((1, 1, tokens)), VMEM],
        out_specs=micro2((1, d_model, tokens)),
        compiler_params=params, cost_estimate=cost,
    )(e, fac, lab, wt)

    per = 2
    head_grad = pl.pallas_call(
        functools.partial(dhead_kernel, inv), name="head_dweight",
        grid=(n_tile, num_micro // per),
        out_shape=jax.ShapeDtypeStruct((vocab, d_model), bf),
        in_specs=[pl.BlockSpec((per, tile, tokens), lambda j, i: (i, j, 0)), pl.BlockSpec((per, n_tile, tokens), lambda j, i: (i, 0, 0)),
                  pl.BlockSpec((per, 1, tokens), lambda j, i: (i, 0, 0)), pl.BlockSpec((per, d_model, tokens), lambda j, i: (i, 0, 0))],
        out_specs=pl.BlockSpec((tile, d_model), lambda j, i: (j, 0)),
        scratch_shapes=[pltpu.VMEM((tile, d_model), f32)],
        compiler_params=params, cost_estimate=cost,
    )(e, fac, lab, n_t)

    dn_own = lax.psum_scatter(dn, 'pp', scatter_dimension=0, tiled=True)
    per_stage = num_micro // n_stage
    h_own = lax.dynamic_slice_in_dim(h_fin, stage_id * per_stage, per_stage, 0).astype(f32)
    r_own = lax.rsqrt(jnp.mean(h_own * h_own, axis=1, keepdims=True) + NORM_EPS)
    n_own = h_own * r_own
    d_fin = r_own * (dn_own - n_own * jnp.mean(dn_own * n_own, axis=1, keepdims=True))
    return loss, head_grad, d_fin.astype(bf)


def bwd_kernel(n_stage, num_micro, dfin_ref, saved_ref, slope_ref, hid_ref, g_ref, w1_ref, w2_ref, dw1_ref, dw2_ref, dg_ref, dx_ref,
               dbuf, obuf, xbuf, h_in, slope_in, hid_in, dpre, acc1, acc2, accg, st1, st2, gb, hrb, dyb, yb,
               in_sem, push_sem, out_sem, x_sem, xr_sem, h_sem, slope_sem, hid_sem, w_sem):
    me = lax.axis_index("pp")
    left = lax.rem(me + n_stage - 1, n_stage)
    first, last = me == 0, me == n_stage - 1
    n_unit = 2 * num_micro
    per = num_micro // n_stage
    d_model, d_ff = w1_ref.shape[1:]
    step = 512
    group_barrier(me, n_stage)

    def fetch(w):
        u, par = n_unit - 1 - w, lax.rem(w, 2)
        return (pltpu.make_async_copy(saved_ref.at[u], h_in.at[par], h_sem.at[par]),
                pltpu.make_async_copy(slope_ref.at[u], slope_in.at[par], slope_sem.at[par]),
                pltpu.make_async_copy(hid_ref.at[u], hid_in.at[par], hid_sem.at[par]))

    for copy in fetch(0):
        copy.start()

    @pl.when(last)
    def _():
        for i in range(per):
            slot = num_micro - 1 - (per * (n_stage - 1) + i)
            pltpu.make_async_copy(dfin_ref.at[i], dbuf.at[slot], in_sem.at[slot]).start()

    @pl.when(jnp.logical_not(last))
    def _():
        for i in reversed(range(per)):
            slot = num_micro - 1 - (per * me + i)
            remote(dfin_ref.at[i], dbuf.at[slot], push_sem.at[i], in_sem.at[slot], n_stage - 1).start()

    @pl.loop(0, n_unit)
    def _(w):
        half = 1 - w // num_micro
        par = lax.rem(w, 2)
        is_local = last & (w < per)
        is_final = first & (half == 0)

        @pl.when(w + 1 < n_unit)
        def _():
            for copy in fetch(w + 1):
                copy.start()

        @pl.when(lax.rem(w, num_micro) == 0)
        def _():
            acc1[...] = jnp.zeros_like(acc1)
            acc2[...] = jnp.zeros_like(acc2)
            accg[...] = jnp.zeros_like(accg)
            gb[...] = jnp.broadcast_to(g_ref[half], gb.shape)

        @pl.when(is_local)
        def _():
            pltpu.make_async_copy(dfin_ref.at[0], dbuf.at[w], in_sem.at[w]).wait()

        @pl.when(jnp.logical_not(is_local))
        def _():
            remote(obuf.at[0], dbuf.at[w], out_sem.at[0], in_sem.at[w], left).wait_recv()

        for copy in fetch(w):
            copy.wait()

        d_in = dbuf[w]
        nxt = nn(w2_ref[half, 0:step, :], d_in)
        for k in range(d_ff // step):
            rows = pl.ds(k * step, step)
            cur = nxt
            if k + 1 < d_ff // step:
                nxt = nn(w2_ref[half, (k + 1) * step:(k + 2) * step, :], d_in)
            dpre[rows, :] = (cur * slope_in[par, rows, :]).astype(jnp.bfloat16)
        h = h_in[par].astype(jnp.float32)
        r = col_scale(h)
        r16 = jnp.broadcast_to(r, (16, r.shape[1]))
        for q in range(0, d_model, 16):
            hr = h_in[par, q:q + 16, :].astype(jnp.float32) * r16
            hrb[q:q + 16, :] = hr
            yb[q:q + 16, :] = (hr * gb[q:q + 16, :]).astype(jnp.bfloat16)
        dyb[...] = nn(w1_ref[half], dpre[...])
        dots = jnp.zeros_like(r16)
        for q in range(0, d_model, 16):
            prod = dyb[q:q + 16, :] * hrb[q:q + 16, :]
            accg[q:q + 16, :] += prod
            dots = dots + prod * gb[q:q + 16, :]
        mean16 = jnp.broadcast_to(jnp.sum(dots, axis=0, keepdims=True) * (1.0 / d_model), r16.shape)
        for q in range(0, d_model, 16):
            dyb[q:q + 16, :] = dbuf[w, q:q + 16, :].astype(jnp.float32) + r16 * (dyb[q:q + 16, :] * gb[q:q + 16, :] - hrb[q:q + 16, :] * mean16)

        @pl.when(is_final)
        def _():
            q = w - num_micro
            slot = lax.rem(q, 4)
            m = num_micro - 1 - q
            owner, i = m // per, lax.rem(m, per)

            @pl.when(q >= 4)
            def _():
                remote(xbuf.at[slot], dx_ref.at[0], x_sem.at[slot], xr_sem.at[0], left).wait_send()

            xbuf[slot] = dyb[...].astype(jnp.bfloat16)

            @pl.when(owner == 0)
            def _():
                pltpu.make_async_copy(xbuf.at[slot], dx_ref.at[i], x_sem.at[slot]).start()

            @pl.when(owner > 0)
            def _():
                remote(xbuf.at[slot], dx_ref.at[i], x_sem.at[slot], xr_sem.at[i], jnp.maximum(owner, 1)).start()

        @pl.when(jnp.logical_not(is_final))
        def _():
            slot = lax.rem(w, 4)

            @pl.when(w >= 4)
            def _():
                remote(obuf.at[slot], dbuf.at[w], out_sem.at[slot], in_sem.at[w], left).wait_send()

            obuf[slot] = dyb[...].astype(jnp.bfloat16)
            dst = w + jnp.where(first, num_micro, 0)
            remote(obuf.at[slot], dbuf.at[dst], out_sem.at[slot], in_sem.at[dst], left).start()

        y = yb[...]
        for k in range(d_ff // step):
            rows = pl.ds(k * step, step)
            acc2[rows, :] += nt(hid_in[par, rows, :], d_in)
            acc1[:, rows] += nt(y, dpre[rows, :])

        @pl.when(lax.rem(w, num_micro) == num_micro - 1)
        def _():
            @pl.when(half == 0)
            def _():
                pltpu.make_async_copy(st1, dw1_ref.at[1], w_sem.at[0]).wait()
                pltpu.make_async_copy(st2, dw2_ref.at[1], w_sem.at[1]).wait()

            st1[...] = acc1[...].astype(jnp.bfloat16)
            st2[...] = acc2[...].astype(jnp.bfloat16)
            dg_ref[half] = jnp.sum(accg[...], axis=1, keepdims=True)
            pltpu.make_async_copy(st1, dw1_ref.at[half], w_sem.at[0]).start()
            pltpu.make_async_copy(st2, dw2_ref.at[half], w_sem.at[1]).start()

    pltpu.make_async_copy(st1, dw1_ref.at[0], w_sem.at[0]).wait()
    pltpu.make_async_copy(st2, dw2_ref.at[0], w_sem.at[1]).wait()
    for slot in range(4):
        remote(obuf.at[slot], dbuf.at[0], out_sem.at[slot], in_sem.at[0], left).wait_send()

    @pl.when(jnp.logical_not(last))
    def _():
        for i in range(per):
            remote(dfin_ref.at[i], dbuf.at[0], push_sem.at[i], in_sem.at[0], n_stage - 1).wait_send()

    @pl.when(first)
    def _():
        remote(xbuf.at[0], dx_ref.at[0], x_sem.at[0], xr_sem.at[0], left).wait_send()
        for slot in range(1, 4):
            pltpu.make_async_copy(xbuf.at[slot], dx_ref.at[0], x_sem.at[slot]).wait()

    @pl.when(jnp.logical_not(first))
    def _():
        for i in range(per):
            remote(xbuf.at[0], dx_ref.at[i], x_sem.at[0], xr_sem.at[i], left).wait_recv()


def run_backward(d_fin, saved, slope, hid, gains, w1, w2, n_stage):
    n_unit, d_model, tokens = saved.shape
    num_micro = n_unit // 2
    d_ff = w1.shape[2]
    per = num_micro // n_stage
    bf, f32 = jnp.bfloat16, jnp.float32
    dma = pltpu.SemaphoreType.DMA
    return pl.pallas_call(
        functools.partial(bwd_kernel, n_stage, num_micro),
        name="stack_bwd",
        out_shape=(jax.ShapeDtypeStruct(w1.shape, bf), jax.ShapeDtypeStruct(w2.shape, bf), jax.ShapeDtypeStruct((2, d_model, 1), f32),
                   jax.ShapeDtypeStruct((per, d_model, tokens), bf)),
        in_specs=[ANY, ANY, ANY, ANY, VMEM, VMEM, VMEM],
        out_specs=(ANY, ANY, VMEM, ANY),
        scratch_shapes=[
            pltpu.VMEM((n_unit, d_model, tokens), bf), pltpu.VMEM((4, d_model, tokens), bf), pltpu.VMEM((4, d_model, tokens), bf),
            pltpu.VMEM((2, d_model, tokens), bf), pltpu.VMEM((2, d_ff, tokens), f32), pltpu.VMEM((2, d_ff, tokens), bf),
            pltpu.VMEM((d_ff, tokens), bf), pltpu.VMEM((d_model, d_ff), f32), pltpu.VMEM((d_ff, d_model), f32), pltpu.VMEM((d_model, tokens), f32),
            pltpu.VMEM((d_model, d_ff), bf), pltpu.VMEM((d_ff, d_model), bf),
            pltpu.VMEM((d_model, tokens), f32), pltpu.VMEM((d_model, tokens), f32), pltpu.VMEM((d_model, tokens), f32), pltpu.VMEM((d_model, tokens), bf),
            dma((n_unit,)), dma((per,)), dma((4,)), dma((4,)), dma((per,)), dma((2,)), dma((2,)), dma((2,)), dma((2,)),
        ],
        compiler_params=pltpu.CompilerParams(collective_id=1, has_side_effects=True, vmem_limit_bytes=VMEM_MAX),
        cost_estimate=pl.CostEstimate(flops=8 * n_unit * tokens * d_model * d_ff, bytes_accessed=7 * n_unit * d_ff * tokens, transcendentals=0),
    )(d_fin, saved, slope, hid, gains, w1, w2)


def solution(mesh):
    n_stage = mesh.shape['pp']

    def local_step(x_embed, labels, norm_gain, w_up, w_down, w_head):
        stage_id = lax.axis_index('pp')
        gains = jnp.swapaxes(norm_gain[0], 1, 2)
        w1, w2 = w_up[0, :, 0], w_down[0, :, 0]
        saved, slope, hid, h_fin, n_t, wt = run_forward(x_embed, gains, w1, w2, w_head, 3, n_stage)
        loss, head_grad, d_fin = run_head(h_fin, n_t, wt, labels, w_head, stage_id, n_stage)
        dw1, dw2, dg, dx = run_backward(d_fin, saved, slope, hid, gains, w1, w2, n_stage)
        return (loss.reshape(1), jnp.swapaxes(dx, 1, 2).astype(jnp.float32), jnp.swapaxes(dg, 1, 2)[None], dw1[None, :, None], dw2[None, :, None], head_grad)

    part_spec = P('dp')
    stage_spec = P('pp')
    out_spec = P(('dp', 'pp'))
    return jax.shard_map(local_step, mesh=mesh, in_specs=(part_spec, part_spec, stage_spec, stage_spec, stage_spec, stage_spec), out_specs=(part_spec, out_spec, out_spec, out_spec, out_spec, out_spec), check_vma=False)
```

```python
import functools

import jax
import jax.numpy as jnp
from jax import lax
from jax.experimental import pallas as pl
from jax.experimental.pallas import tpu as pltpu
from jax.sharding import PartitionSpec as P

NORM_EPS = 1e-6
VMEM_MAX = 67_000_000
GELU_A = 0.7978845608028654
GELU_B = GELU_A * 0.044715
SUB = 1024
RANGE = 40.0

ANY = pl.BlockSpec(memory_space=pl.ANY)
VMEM = pl.BlockSpec(memory_space=pltpu.VMEM)


def nn(lhs, rhs):
    return lax.dot_general(lhs, rhs, (((1,), (0,)), ((), ())), preferred_element_type=jnp.float32)


def nt(lhs, rhs):
    return lax.dot_general(lhs, rhs, (((1,), (1,)), ((), ())), preferred_element_type=jnp.float32)


def col_scale(h_f32):
    return lax.rsqrt(jnp.mean(h_f32 * h_f32, axis=0, keepdims=True) + NORM_EPS)


def gelu_pair(x):
    x2 = x * x
    th = jnp.tanh(x * (GELU_A + GELU_B * x2))
    hx = 0.5 * x
    slope = 0.5 + 0.5 * th + hx * (1.0 - th * th) * (GELU_A + (3.0 * GELU_B) * x2)
    return hx + hx * th, slope


def group_barrier(me, n_stage):
    sem = pltpu.get_barrier_semaphore()
    for step in range(1, n_stage):
        pl.semaphore_signal(sem, inc=1, device_id={"pp": lax.rem(me + step, n_stage)}, device_id_type=pl.DeviceIdType.MESH)
    pl.semaphore_wait(sem, n_stage - 1)


def remote(src, dst, send_sem, recv_sem, dev):
    return pltpu.make_async_remote_copy(src_ref=src, dst_ref=dst, send_sem=send_sem, recv_sem=recv_sem, device_id={"pp": dev}, device_id_type=pl.DeviceIdType.MESH)


def fwd_kernel(n_stage, num_micro, x_ref, g_ref, w1_ref, w2_ref, wh_ref, saved_ref, slope_ref, hid_ref, hfin_ref, n_ref, wht_ref,
               w1t, w2t, hbuf, obuf, fbuf, slope_st, hid_st, wh_in, wh_out, wh_last, wht_last, in_sem, out_sem, save_sem, slope_sem, hid_sem, fin_sem, fin_a, fin_b, fin_c, whi_sem, who_sem):
    me = lax.axis_index("pp")
    right = lax.rem(me + 1, n_stage)
    first, last = me == 0, me == n_stage - 1
    n_unit = 2 * num_micro
    d_ff = w1_ref.shape[2]
    n_tile, tile = wht_ref.shape[0], wht_ref.shape[2]
    subs = sub_tiles(tile)
    group_barrier(me, n_stage)

    def emit_norm(m):
        hf = fbuf[m].astype(jnp.float32)
        hbuf[m] = (hf * col_scale(hf)).astype(jnp.bfloat16)
        pltpu.make_async_copy(hbuf.at[m], n_ref.at[m], save_sem.at[m]).start()

    def head_copies(t, k):
        off, size = subs[k]
        last_sub = k + 1 == len(subs)
        src, dst = (wh_last, wht_last) if last_sub else (wh_in, wh_out)
        rows = pl.ds(pl.multiple_of(t * tile + off, 16), size)
        return (src, dst, lambda: pltpu.make_async_copy(wh_ref.at[rows, :], src, whi_sem.at[int(last_sub)]),
                lambda: pltpu.make_async_copy(dst, wht_ref.at[t, :, off:off + size], who_sem.at[int(last_sub)]))

    @pl.when(first)
    def _():
        @pl.loop(0, num_micro)
        def _(m):
            pltpu.make_async_copy(x_ref.at[m], hbuf.at[m], in_sem.at[m]).start()

    @pl.loop(0, n_unit)
    def _(u):
        half = u // num_micro

        @pl.when(lax.rem(u, num_micro) == 0)
        def _():
            w1t[...] = w1_ref[half].T
            w2t[...] = w2_ref[half].T

        m = lax.rem(u, num_micro)
        from_x = first & (half == 0)
        is_final = last & (half == 1)
        par = lax.rem(u, 2)

        @pl.when(from_x)
        def _():
            pltpu.make_async_copy(x_ref.at[m], hbuf.at[u], in_sem.at[u]).wait()
            hbuf[u] = hbuf[u].T

        @pl.when(jnp.logical_not(from_x))
        def _():
            remote(obuf.at[0], hbuf.at[u], out_sem.at[0], in_sem.at[u], right).wait_recv()

        pltpu.make_async_copy(hbuf.at[u], saved_ref.at[u], save_sem.at[u]).start()

        @pl.when(u >= 2)
        def _():
            pltpu.make_async_copy(slope_st.at[par], slope_ref.at[u - 2], slope_sem.at[par]).wait()
            pltpu.make_async_copy(hid_st.at[par], hid_ref.at[u - 2], hid_sem.at[par]).wait()

        h = hbuf[u].astype(jnp.float32)
        y = (h * col_scale(h) * g_ref[half]).astype(jnp.bfloat16)
        step = 512
        pre = nn(w1t[0:step, :], y)
        for k in range(d_ff // step):
            rows = pl.ds(k * step, step)
            cur = pre
            if k + 1 < d_ff // step:
                pre = nn(w1t[(k + 1) * step:(k + 2) * step, :], y)
            hid, slope = gelu_pair(cur)
            hid_st[par, rows, :] = hid.astype(jnp.bfloat16)
            slope_st[par, rows, :] = slope
        out = (h + nn(w2t[...], hid_st[par])).astype(jnp.bfloat16)
        pltpu.make_async_copy(slope_st.at[par], slope_ref.at[u], slope_sem.at[par]).start()
        pltpu.make_async_copy(hid_st.at[par], hid_ref.at[u], hid_sem.at[par]).start()

        @pl.when(is_final)
        def _():
            fbuf[m] = out
            pltpu.make_async_copy(fbuf.at[m], hfin_ref.at[m], fin_c.at[m]).start()
            remote(fbuf.at[m], fbuf.at[m], fin_a.at[m], fin_sem.at[m], n_stage - 2).start()
            remote(fbuf.at[m], fbuf.at[m], fin_b.at[m], fin_sem.at[m], 1).start()
            pltpu.make_async_copy(hbuf.at[m], saved_ref.at[m], save_sem.at[m]).wait()
            emit_norm(m)

        @pl.when(jnp.logical_not(is_final))
        def _():
            slot = lax.rem(u, 4)

            @pl.when(u >= 4)
            def _():
                remote(obuf.at[slot], hbuf.at[u], out_sem.at[slot], in_sem.at[u], right).wait_send()

            obuf[slot] = out
            dst = u + jnp.where(last, num_micro, 0)
            remote(obuf.at[slot], hbuf.at[dst], out_sem.at[slot], in_sem.at[dst], right).start()

        for k in range(len(subs)):
            @pl.when((lax.rem(u, 2 * len(subs)) == 2 * k) & (u // (2 * len(subs)) < n_tile))
            def _(k=k):
                head_copies(u // (2 * len(subs)), k)[2]().start()

            @pl.when((lax.rem(u, 2 * len(subs)) == 2 * k + 1) & (u // (2 * len(subs)) < n_tile))
            def _(k=k):
                t = u // (2 * len(subs))
                src, dst, copy_in, copy_out = head_copies(t, k)
                copy_in().wait()
                if k in (0, len(subs) - 1):
                    @pl.when(t > 0)
                    def _():
                        copy_out().wait()
                else:
                    copy_out().wait()
                dst[...] = src[...].T
                copy_out().start()

    for k in (0, len(subs) - 1):
        head_copies(0, k)[3]().wait()
    for slot in range(4):
        remote(obuf.at[slot], hbuf.at[0], out_sem.at[slot], in_sem.at[0], right).wait_send()
    for par in range(2):
        pltpu.make_async_copy(slope_st.at[par], slope_ref.at[par], slope_sem.at[par]).wait()
        pltpu.make_async_copy(hid_st.at[par], hid_ref.at[par], hid_sem.at[par]).wait()

    @pl.loop(0, n_unit)
    def _(u):
        pltpu.make_async_copy(hbuf.at[u], saved_ref.at[u], save_sem.at[u]).wait()

    @pl.when(last)
    def _():
        @pl.loop(0, num_micro)
        def _(m):
            pltpu.make_async_copy(fbuf.at[m], hfin_ref.at[m], fin_c.at[m]).wait()
            remote(fbuf.at[m], fbuf.at[m], fin_a.at[m], fin_sem.at[m], n_stage - 2).wait_send()
            remote(fbuf.at[m], fbuf.at[m], fin_b.at[m], fin_sem.at[m], 1).wait_send()

    @pl.when(jnp.logical_not(last))
    def _():
        @pl.loop(0, num_micro)
        def _(m):
            remote(fbuf.at[m], fbuf.at[m], fin_a.at[m], fin_sem.at[m], right).wait_recv()

            @pl.when(me == 1)
            def _():
                remote(fbuf.at[m], fbuf.at[m], fin_a.at[m], fin_sem.at[m], 0).start()

            pltpu.make_async_copy(fbuf.at[m], hfin_ref.at[m], fin_c.at[m]).start()
            emit_norm(m)

        @pl.loop(0, num_micro)
        def _(m):
            pltpu.make_async_copy(fbuf.at[m], hfin_ref.at[m], fin_c.at[m]).wait()
            pltpu.make_async_copy(hbuf.at[m], n_ref.at[m], save_sem.at[m]).wait()

    @pl.when(me == 1)
    def _():
        @pl.loop(0, num_micro)
        def _(m):
            remote(fbuf.at[m], fbuf.at[m], fin_a.at[m], fin_sem.at[m], 0).wait_send()


def run_forward(x_embed, gains, w1, w2, w_head, n_tile, n_stage):
    num_micro, tokens, d_model = x_embed.shape
    d_ff = w1.shape[2]
    bf, f32 = jnp.bfloat16, jnp.float32
    n_unit = 2 * num_micro
    tile = w_head.shape[0] // n_tile
    last_rows = sub_tiles(tile)[-1][1]
    dma = pltpu.SemaphoreType.DMA
    return pl.pallas_call(
        functools.partial(fwd_kernel, n_stage, num_micro),
        name="stack_fwd",
        out_shape=(jax.ShapeDtypeStruct((n_unit, d_model, tokens), bf), jax.ShapeDtypeStruct((n_unit, d_ff, tokens), f32),
                   jax.ShapeDtypeStruct((n_unit, d_ff, tokens), bf), jax.ShapeDtypeStruct((num_micro, d_model, tokens), bf),
                   jax.ShapeDtypeStruct((num_micro, d_model, tokens), bf), jax.ShapeDtypeStruct((n_tile, d_model, tile), bf)),
        in_specs=[ANY, VMEM, VMEM, VMEM, ANY],
        out_specs=(ANY, ANY, ANY, ANY, ANY, ANY),
        scratch_shapes=[
            pltpu.VMEM((d_ff, d_model), bf), pltpu.VMEM((d_model, d_ff), bf),
            pltpu.VMEM((n_unit, d_model, tokens), bf), pltpu.VMEM((4, d_model, tokens), bf), pltpu.VMEM((num_micro, d_model, tokens), bf),
            pltpu.VMEM((2, d_ff, tokens), f32), pltpu.VMEM((2, d_ff, tokens), bf),
            pltpu.VMEM((SUB, d_model), bf), pltpu.VMEM((d_model, SUB), bf), pltpu.VMEM((last_rows, d_model), bf), pltpu.VMEM((d_model, last_rows), bf),
            dma((n_unit,)), dma((4,)), dma((n_unit,)), dma((2,)), dma((2,)), dma((num_micro,)), dma((num_micro,)), dma((num_micro,)), dma((num_micro,)),
            dma((2,)), dma((2,)),
        ],
        compiler_params=pltpu.CompilerParams(collective_id=0, has_side_effects=True, vmem_limit_bytes=VMEM_MAX),
        cost_estimate=pl.CostEstimate(flops=4 * n_unit * tokens * d_model * d_ff, bytes_accessed=7 * n_unit * d_ff * tokens, transcendentals=0),
    )(x_embed, gains, w1, w2, w_head)


def sub_tiles(tile):
    n_sub = tile // SUB
    return [(k * SUB, SUB if k + 1 < n_sub else tile - k * SUB) for k in range(n_sub)]


def logits_kernel(tile, n_ref, lab_ref, w_ref, e_ref, mrun_ref, stat_ref, used, s_buf):
    vocab, tokens = e_ref.shape[1], e_ref.shape[2]
    n_tile = vocab // tile
    piece, small = 256, 32
    n = n_ref[0]
    lab = lab_ref[0]
    group = jnp.where(lax.broadcasted_iota(jnp.int32, (8, tokens), 0) == (lab & 7), lab >> 3, -1)

    def rows_at(t, off, size):
        return pl.ds(pl.multiple_of(t * tile + off, 16), size)

    def body(t, carry):
        m_run, s_run, hit = carry
        m_use = jnp.where(t == 0, 0.0, m_run)
        m8 = jnp.broadcast_to(m_use, (8, tokens))
        top = jnp.full((8, tokens), -jnp.inf, jnp.float32)
        s8 = jnp.zeros((8, tokens), jnp.float32)
        local = group - t * (tile // 8)
        n_piece = tile // piece
        for q in range(n_piece):
            off = q * piece
            size = piece if q + 1 < n_piece else tile - off
            z = nn(w_ref[rows_at(t, off, size), :], n)
            for r in range(0, size, 16):
                e = []
                for g in range(2):
                    zg = z[r + 8 * g:r + 8 * g + 8, :]
                    top = jnp.maximum(top, zg)
                    hit = jnp.where(local == (off + r) // 8 + g, zg, hit)
                    e.append(jnp.exp(zg - m8))
                    s8 = s8 + e[g]
                e_ref[0, rows_at(t, off + r, 16), :] = jnp.concatenate(e, axis=0).astype(jnp.bfloat16)
        m_new = jnp.maximum(m_run, jnp.max(top, axis=0, keepdims=True))
        used[0:1, :] = m_use
        s_buf[...] = s8
        rise = jnp.max(m_new - m_use)
        fall = jnp.max(m_use - m_new)

        @pl.when((rise > RANGE) | (fall > RANGE))
        def _():
            used[0:1, :] = m_new
            s_buf[...] = jnp.zeros_like(s_buf)

            @pl.loop(0, tile // small)
            def _(q):
                e = jnp.exp(nn(w_ref[rows_at(t, q * small, small), :], n) - m_new)
                e_ref[0, rows_at(t, q * small, small), :] = e.astype(jnp.bfloat16)
                for r in range(0, small, 8):
                    s_buf[...] += e[r:r + 8, :]

        m_use = used[0:1, :]
        mrun_ref[0, pl.ds(t, 1), :] = m_use
        s_run = s_run * jnp.exp(m_run - m_new) + s_buf[...] * jnp.exp(m_use - m_new)
        return m_new, s_run, hit

    low = jnp.full((1, tokens), -jnp.inf, jnp.float32)
    zero = jnp.zeros((8, tokens), jnp.float32)
    m, s8, hit = lax.fori_loop(0, n_tile, body, (low, zero, zero))
    stat_ref[0, 0:1, :] = m
    stat_ref[0, 1:2, :] = jnp.sum(s8, axis=0, keepdims=True)
    stat_ref[0, 2:3, :] = jnp.sum(hit, axis=0, keepdims=True)


def d_logits(e_tile, fac_row, lab, off, inv):
    hit = lax.broadcasted_iota(jnp.int32, e_tile.shape, 0) == lab - off
    return (e_tile.astype(jnp.float32) * fac_row - jnp.where(hit, inv, 0.0)).astype(jnp.bfloat16)


def dnorm_kernel(inv, e_ref, fac_ref, lab_ref, wt_ref, dn_ref):
    j = pl.program_id(1)
    tile = e_ref.shape[1]
    subs = sub_tiles(tile)
    lab = lab_ref[0] - j * tile
    total = None
    for k, (off, size) in enumerate(subs):
        d = d_logits(e_ref[0, off:off + size, :], fac_ref[0, pl.ds(j, 1), :], lab, off, inv)
        part = nn(wt_ref[j, :, off:off + size], d)
        total = part if total is None else total + part

    @pl.when(j == 0)
    def _():
        dn_ref[0] = total

    @pl.when(j > 0)
    def _():
        dn_ref[0] += total


def dhead_kernel(inv, e_ref, fac_ref, lab_ref, n_ref, out_ref, acc):
    j, i = pl.program_id(0), pl.program_id(1)
    tile = e_ref.shape[1]
    subs = sub_tiles(tile)
    per = e_ref.shape[0]

    @pl.when(i == 0)
    def _():
        acc[...] = jnp.zeros_like(acc)

    for k, (off, size) in enumerate(subs):
        total = None
        for b in range(per):
            d = d_logits(e_ref[b, off:off + size, :], fac_ref[b, pl.ds(j, 1), :], lab_ref[b] - j * tile, off, inv)
            part = nt(d, n_ref[b])
            total = part if total is None else total + part
        acc[off:off + size, :] += total

    @pl.when(i == pl.num_programs(1) - 1)
    def _():
        out_ref[...] = acc[...].astype(jnp.bfloat16)


def run_head(h_fin, n_t, wt, labels, w_head, stage_id, n_stage):
    num_micro, d_model, tokens = h_fin.shape
    vocab = w_head.shape[0]
    n_tile, tile = wt.shape[0], wt.shape[2]
    n_row = 8
    bf, f32 = jnp.bfloat16, jnp.float32
    inv = 1.0 / (num_micro * tokens)
    lab = (labels - stage_id * vocab).reshape(num_micro, 1, tokens)
    params = pltpu.CompilerParams(vmem_limit_bytes=VMEM_MAX)
    cost = pl.CostEstimate(flops=2 * num_micro * tokens * d_model * vocab, bytes_accessed=2 * num_micro * tokens * vocab, transcendentals=0)

    def micro(shape):
        return pl.BlockSpec(shape, lambda i: (i, 0, 0))

    def micro2(shape):
        return pl.BlockSpec(shape, lambda i, j: (i, 0, 0))

    e, m_run, stat = pl.pallas_call(
        functools.partial(logits_kernel, tile), name="head_logits",
        grid=(num_micro,),
        out_shape=(jax.ShapeDtypeStruct((num_micro, vocab, tokens), bf), jax.ShapeDtypeStruct((num_micro, n_row, tokens), f32),
                   jax.ShapeDtypeStruct((num_micro, 8, tokens), f32)),
        in_specs=[micro((1, d_model, tokens)), micro((1, 1, tokens)), VMEM],
        out_specs=(micro((1, vocab, tokens)), micro((1, n_row, tokens)), micro((1, 8, tokens))),
        scratch_shapes=[pltpu.VMEM((8, tokens), f32), pltpu.VMEM((8, tokens), f32)],
        compiler_params=params, cost_estimate=cost,
    )(n_t, lab, w_head)

    stats = lax.all_gather(stat[:, :3, :], 'pp')
    m_all, s_all = stats[:, :, 0], stats[:, :, 1]
    m_top = jnp.max(m_all, axis=0)
    s_top = jnp.sum(s_all * jnp.exp(m_all - m_top), axis=0)
    loss = jnp.sum(m_top + jnp.log(s_top) - jnp.sum(stats[:, :, 2], axis=0)) * inv
    fac = jnp.exp(m_run[:, :n_tile] - m_top[:, None, :]) * (inv / s_top)[:, None, :]

    dn = pl.pallas_call(
        functools.partial(dnorm_kernel, inv), name="head_dnorm",
        grid=(num_micro, n_tile),
        out_shape=jax.ShapeDtypeStruct((num_micro, d_model, tokens), f32),
        in_specs=[pl.BlockSpec((1, tile, tokens), lambda i, j: (i, j, 0)), micro2((1, n_tile, tokens)), micro2((1, 1, tokens)), VMEM],
        out_specs=micro2((1, d_model, tokens)),
        compiler_params=params, cost_estimate=cost,
    )(e, fac, lab, wt)

    per = 2
    head_grad = pl.pallas_call(
        functools.partial(dhead_kernel, inv), name="head_dweight",
        grid=(n_tile, num_micro // per),
        out_shape=jax.ShapeDtypeStruct((vocab, d_model), bf),
        in_specs=[pl.BlockSpec((per, tile, tokens), lambda j, i: (i, j, 0)), pl.BlockSpec((per, n_tile, tokens), lambda j, i: (i, 0, 0)),
                  pl.BlockSpec((per, 1, tokens), lambda j, i: (i, 0, 0)), pl.BlockSpec((per, d_model, tokens), lambda j, i: (i, 0, 0))],
        out_specs=pl.BlockSpec((tile, d_model), lambda j, i: (j, 0)),
        scratch_shapes=[pltpu.VMEM((tile, d_model), f32)],
        compiler_params=params, cost_estimate=cost,
    )(e, fac, lab, n_t)

    dn_own = lax.psum_scatter(dn, 'pp', scatter_dimension=0, tiled=True)
    per_stage = num_micro // n_stage
    h_own = lax.dynamic_slice_in_dim(h_fin, stage_id * per_stage, per_stage, 0).astype(f32)
    r_own = lax.rsqrt(jnp.mean(h_own * h_own, axis=1, keepdims=True) + NORM_EPS)
    n_own = h_own * r_own
    d_fin = r_own * (dn_own - n_own * jnp.mean(dn_own * n_own, axis=1, keepdims=True))
    return loss, head_grad, d_fin.astype(bf)


def bwd_kernel(n_stage, num_micro, dfin_ref, saved_ref, slope_ref, hid_ref, g_ref, w1_hbm, w2_hbm, dw1_ref, dw2_ref, dg_ref, dx_ref,
               dbuf, obuf, xbuf, h_in, slope_in, hid_in, dpre, acc1, acc2, accg, st1, st2, gb, hrb, dyb, yb, w1_ref, w2_ref,
               in_sem, push_sem, out_sem, x_sem, xr_sem, h_sem, slope_sem, hid_sem, w_sem, wl_sem):
    me = lax.axis_index("pp")
    left = lax.rem(me + n_stage - 1, n_stage)
    first, last = me == 0, me == n_stage - 1
    n_unit = 2 * num_micro
    per = num_micro // n_stage
    d_model, d_ff = w1_ref.shape[1:]
    step = 1024

    def weights(half):
        return (pltpu.make_async_copy(w1_hbm.at[half], w1_ref.at[half], wl_sem.at[half, 0]),
                pltpu.make_async_copy(w2_hbm.at[half], w2_ref.at[half], wl_sem.at[half, 1]))

    for half in (1, 0):
        for copy in weights(half):
            copy.start()
    group_barrier(me, n_stage)

    def fetch(w):
        u, par = n_unit - 1 - w, lax.rem(w, 2)
        return (pltpu.make_async_copy(saved_ref.at[u], h_in.at[par], h_sem.at[par]),
                pltpu.make_async_copy(slope_ref.at[u], slope_in.at[par], slope_sem.at[par]),
                pltpu.make_async_copy(hid_ref.at[u], hid_in.at[par], hid_sem.at[par]))

    for copy in fetch(0):
        copy.start()

    @pl.when(last)
    def _():
        for i in range(per):
            slot = num_micro - 1 - (per * (n_stage - 1) + i)
            pltpu.make_async_copy(dfin_ref.at[i], dbuf.at[slot], in_sem.at[slot]).start()

    @pl.when(jnp.logical_not(last))
    def _():
        for i in reversed(range(per)):
            slot = num_micro - 1 - (per * me + i)
            remote(dfin_ref.at[i], dbuf.at[slot], push_sem.at[i], in_sem.at[slot], n_stage - 1).start()

    @pl.loop(0, n_unit)
    def _(w):
        half = 1 - w // num_micro
        par = lax.rem(w, 2)
        is_local = last & (w < per)
        is_final = first & (half == 0)

        @pl.when(w + 1 < n_unit)
        def _():
            for copy in fetch(w + 1):
                copy.start()

        @pl.when(lax.rem(w, num_micro) == 0)
        def _():
            acc1[...] = jnp.zeros_like(acc1)
            acc2[...] = jnp.zeros_like(acc2)
            accg[...] = jnp.zeros_like(accg)
            for copy in weights(half):
                copy.wait()
            gb[...] = jnp.broadcast_to(g_ref[half], gb.shape)

        @pl.when(is_local)
        def _():
            pltpu.make_async_copy(dfin_ref.at[0], dbuf.at[w], in_sem.at[w]).wait()

        @pl.when(jnp.logical_not(is_local))
        def _():
            remote(obuf.at[0], dbuf.at[w], out_sem.at[0], in_sem.at[w], left).wait_recv()

        for copy in fetch(w):
            copy.wait()

        d_in = dbuf[w]
        nxt = nn(w2_ref[half, 0:step, :], d_in)
        for k in range(d_ff // step):
            rows = pl.ds(k * step, step)
            cur = nxt
            if k + 1 < d_ff // step:
                nxt = nn(w2_ref[half, (k + 1) * step:(k + 2) * step, :], d_in)
            dpre[rows, :] = (cur * slope_in[par, rows, :]).astype(jnp.bfloat16)
        h = h_in[par].astype(jnp.float32)
        r = col_scale(h)
        r16 = jnp.broadcast_to(r, (16, r.shape[1]))
        for q in range(0, d_model, 16):
            hr = h_in[par, q:q + 16, :].astype(jnp.float32) * r16
            hrb[q:q + 16, :] = hr
            yb[q:q + 16, :] = (hr * gb[q:q + 16, :]).astype(jnp.bfloat16)
        dyb[...] = nn(w1_ref[half], dpre[...])
        dots = jnp.zeros_like(r16)
        for q in range(0, d_model, 16):
            prod = dyb[q:q + 16, :] * hrb[q:q + 16, :]
            accg[q:q + 16, :] += prod
            dots = dots + prod * gb[q:q + 16, :]
        mean16 = jnp.broadcast_to(jnp.sum(dots, axis=0, keepdims=True) * (1.0 / d_model), r16.shape)
        for q in range(0, d_model, 16):
            dyb[q:q + 16, :] = dbuf[w, q:q + 16, :].astype(jnp.float32) + r16 * (dyb[q:q + 16, :] * gb[q:q + 16, :] - hrb[q:q + 16, :] * mean16)

        @pl.when(is_final)
        def _():
            q = w - num_micro
            slot = lax.rem(q, 4)
            m = num_micro - 1 - q
            owner, i = m // per, lax.rem(m, per)

            @pl.when(q >= 4)
            def _():
                remote(xbuf.at[slot], dx_ref.at[0], x_sem.at[slot], xr_sem.at[0], left).wait_send()

            xbuf[slot] = dyb[...].astype(jnp.bfloat16)

            @pl.when(owner == 0)
            def _():
                pltpu.make_async_copy(xbuf.at[slot], dx_ref.at[i], x_sem.at[slot]).start()

            @pl.when(owner > 0)
            def _():
                remote(xbuf.at[slot], dx_ref.at[i], x_sem.at[slot], xr_sem.at[i], jnp.maximum(owner, 1)).start()

        @pl.when(jnp.logical_not(is_final))
        def _():
            slot = lax.rem(w, 4)

            @pl.when(w >= 4)
            def _():
                remote(obuf.at[slot], dbuf.at[w], out_sem.at[slot], in_sem.at[w], left).wait_send()

            obuf[slot] = dyb[...].astype(jnp.bfloat16)
            dst = w + jnp.where(first, num_micro, 0)
            remote(obuf.at[slot], dbuf.at[dst], out_sem.at[slot], in_sem.at[dst], left).start()

        acc2[...] += nt(hid_in[par], d_in)
        acc1[...] += nt(dpre[...], yb[...])

        @pl.when(lax.rem(w, num_micro) == num_micro - 1)
        def _():
            @pl.when(half == 0)
            def _():
                pltpu.make_async_copy(st1, dw1_ref.at[1], w_sem.at[0]).wait()
                pltpu.make_async_copy(st2, dw2_ref.at[1], w_sem.at[1]).wait()

            st1[...] = acc1[...].astype(jnp.bfloat16).T
            st2[...] = acc2[...].astype(jnp.bfloat16)
            dg_ref[half] = jnp.sum(accg[...], axis=1, keepdims=True)
            pltpu.make_async_copy(st1, dw1_ref.at[half], w_sem.at[0]).start()
            pltpu.make_async_copy(st2, dw2_ref.at[half], w_sem.at[1]).start()

    pltpu.make_async_copy(st1, dw1_ref.at[0], w_sem.at[0]).wait()
    pltpu.make_async_copy(st2, dw2_ref.at[0], w_sem.at[1]).wait()
    for slot in range(4):
        remote(obuf.at[slot], dbuf.at[0], out_sem.at[slot], in_sem.at[0], left).wait_send()

    @pl.when(jnp.logical_not(last))
    def _():
        for i in range(per):
            remote(dfin_ref.at[i], dbuf.at[0], push_sem.at[i], in_sem.at[0], n_stage - 1).wait_send()

    @pl.when(first)
    def _():
        remote(xbuf.at[0], dx_ref.at[0], x_sem.at[0], xr_sem.at[0], left).wait_send()
        for slot in range(1, 4):
            pltpu.make_async_copy(xbuf.at[slot], dx_ref.at[0], x_sem.at[slot]).wait()

    @pl.when(jnp.logical_not(first))
    def _():
        for i in range(per):
            remote(xbuf.at[0], dx_ref.at[i], x_sem.at[0], xr_sem.at[i], left).wait_recv()


def run_backward(d_fin, saved, slope, hid, gains, w1, w2, n_stage):
    n_unit, d_model, tokens = saved.shape
    num_micro = n_unit // 2
    d_ff = w1.shape[2]
    per = num_micro // n_stage
    bf, f32 = jnp.bfloat16, jnp.float32
    dma = pltpu.SemaphoreType.DMA
    return pl.pallas_call(
        functools.partial(bwd_kernel, n_stage, num_micro),
        name="stack_bwd",
        out_shape=(jax.ShapeDtypeStruct(w1.shape, bf), jax.ShapeDtypeStruct(w2.shape, bf), jax.ShapeDtypeStruct((2, d_model, 1), f32),
                   jax.ShapeDtypeStruct((per, d_model, tokens), bf)),
        in_specs=[ANY, ANY, ANY, ANY, VMEM, ANY, ANY],
        out_specs=(ANY, ANY, VMEM, ANY),
        scratch_shapes=[
            pltpu.VMEM((n_unit, d_model, tokens), bf), pltpu.VMEM((4, d_model, tokens), bf), pltpu.VMEM((4, d_model, tokens), bf),
            pltpu.VMEM((2, d_model, tokens), bf), pltpu.VMEM((2, d_ff, tokens), f32), pltpu.VMEM((2, d_ff, tokens), bf),
            pltpu.VMEM((d_ff, tokens), bf), pltpu.VMEM((d_ff, d_model), f32), pltpu.VMEM((d_ff, d_model), f32), pltpu.VMEM((d_model, tokens), f32),
            pltpu.VMEM((d_model, d_ff), bf), pltpu.VMEM((d_ff, d_model), bf),
            pltpu.VMEM((d_model, tokens), f32), pltpu.VMEM((d_model, tokens), f32), pltpu.VMEM((d_model, tokens), f32), pltpu.VMEM((d_model, tokens), bf),
            pltpu.VMEM(w1.shape, bf), pltpu.VMEM(w2.shape, bf),
            dma((n_unit,)), dma((per,)), dma((4,)), dma((4,)), dma((per,)), dma((2,)), dma((2,)), dma((2,)), dma((2,)), dma((2, 2)),
        ],
        compiler_params=pltpu.CompilerParams(collective_id=1, has_side_effects=True, vmem_limit_bytes=VMEM_MAX),
        cost_estimate=pl.CostEstimate(flops=8 * n_unit * tokens * d_model * d_ff, bytes_accessed=7 * n_unit * d_ff * tokens, transcendentals=0),
    )(d_fin, saved, slope, hid, gains, w1, w2)


def solution(mesh):
    n_stage = mesh.shape['pp']

    def local_step(x_embed, labels, norm_gain, w_up, w_down, w_head):
        stage_id = lax.axis_index('pp')
        gains = jnp.swapaxes(norm_gain[0], 1, 2)
        w1, w2 = w_up[0, :, 0], w_down[0, :, 0]
        saved, slope, hid, h_fin, n_t, wt = run_forward(x_embed, gains, w1, w2, w_head, 3, n_stage)
        loss, head_grad, d_fin = run_head(h_fin, n_t, wt, labels, w_head, stage_id, n_stage)
        dw1, dw2, dg, dx = run_backward(d_fin, saved, slope, hid, gains, w1, w2, n_stage)
        return (loss.reshape(1), jnp.swapaxes(dx, 1, 2).astype(jnp.float32), jnp.swapaxes(dg, 1, 2)[None], dw1[None, :, None], dw2[None, :, None], head_grad)

    part_spec = P('dp')
    stage_spec = P('pp')
    out_spec = P(('dp', 'pp'))
    return jax.shard_map(local_step, mesh=mesh, in_specs=(part_spec, part_spec, stage_spec, stage_spec, stage_spec, stage_spec), out_specs=(part_spec, out_spec, out_spec, out_spec, out_spec, out_spec), check_vma=False)
```
